32 devices in a mesh: tm: 2 (over core), space: 16 (over z, y, x).
Axes of the slice: x: 2, y: 2, z: 4, core: 2. Of those that a mesh axis runs over, the one named last changes fastest.
Arguments:
- checkpoints: float32 [2, 5, 2048, 128], P('tm', None, 'space'), may hold values from -6 to 6
- sources: float32 [2, 5, 2048, 128], P(None, None, 'space'), may hold values from -3 to 3
- pitch: float32 [8], replicated, may hold values from -3.140625 to 3.140625
- metric: float32 [2048, 128], P('space'), may hold values from 0.5 to 2
- obj_weight: float32 [5, 2048, 128], P(None, 'space'), may hold values from 0.1 to 0.6
- adjoint_end: float32 [5, 2048, 128], P(None, 'space'), may hold values from -6 to 6
- lift: bfloat16 [5, 128, 128], replicated, may hold values from -0.5 to 0.5
- mixing: float32 [5, 5, 5], replicated, may hold values from -1.25 to 1.25
- faces: int32 [2048, 4], P('space'), may hold values from 0 to 191
- send_idx: int32 [16, 4, 16], P('space'), may hold values from 0 to 127
Outputs:
- adjoint_bounds: float32 [2, 5, 2048, 128], P('tm', None, 'space')
- pitch_grad: float32 [8], replicated
The draws below stay inside these ranges and needn't reach their ends.
Inputs may be any that keep to these rules, and one draw needn't show every extreme that they name: `faces`: values below 128 name the subdomain's own blocks; value 128 + d * 16 + s names slot s of the blocks received from direction d. `send_idx`: entry [p, d, s] is a local block of subdomain p sent to subdomain p + o[d], o = (1, -1, 2, -2); blocks may repeat.
All inputs are finite; a program needn't handle non-finite values.
Results may differ from the reference program's by a relative error of at most 0.0035.
Values may be sent and summed in bfloat16 or wider, within the bound.
A program may use at most 64 MiB of HBM per device.

```python
import math
import jax
import jax.numpy as jnp
from jax import lax

COMPS = 5
NODES = 128
FACES = 4
LEVELS = 8
BLK_DEV = 128
HALO = 16
NBT = 2048
N_TM = 2
N_SPACE = 16


def with_ends(drawn, key, least, high):
    extent = drawn.shape
    spot = [jax.random.randint(jax.random.fold_in(key, axis), (), 0, extent[axis]) for axis in range(len(extent))]
    drawn = drawn.at[tuple(spot)].set(least)
    longest = extent.index(max(extent))
    spot[longest] = (spot[longest] + 1) % extent[longest]
    return drawn.at[tuple(spot)].set(high)


def level_of(rng, extent, cuts, low, largest):
    factor_of, own = 1.0, jax.random.fold_in(rng, 6)
    for position, blocks in cuts:
        steps = jnp.exp(jax.random.uniform(jax.random.fold_in(own, position), (blocks,), jnp.float32, low / len(cuts), largest / len(cuts)))
        factor_of = factor_of * jnp.repeat(steps, extent[position] // blocks).reshape([-1 if axis == position else 1 for axis in range(len(extent))])
    return factor_of


def noise(rng, dims, spread, limit, cuts=(), held_as=jnp.bfloat16):
    entries = jax.random.normal(rng, dims, jnp.float32) * spread
    if len(cuts) > 0:
        entries = level_of(rng, dims, cuts, -0.22, 0.18) * entries
    return jnp.clip(entries, min=-limit, max=limit).astype(held_as)


def setup_inputs(seed: int = 0) -> dict:
    key_of = jax.random.split(jax.random.key(seed), 11)
    return {
        "checkpoints": noise(key_of[0], (2, COMPS, NBT, NODES), 1.0, 6.0, ((0, 2), (2, 16)), jnp.float32),
        "sources": noise(key_of[1], (2, COMPS, NBT, NODES), 0.5, 3.0, ((2, 16),), jnp.float32),
        "pitch": jnp.clip(jax.random.uniform(key_of[2], (LEVELS,), jnp.float32, -3.140625, 3.140625), -3.140625, 3.140625),
        "metric": jnp.clip(jnp.exp(math.log(2.0) - 1.3862944 * jax.random.uniform(key_of[3], (NBT, NODES), jnp.float32) ** level_of(key_of[3], (NBT, NODES), ((0, 16),), -0.2, 0.2)), 0.5, 2.0),
        "obj_weight": jnp.clip(0.1 + 0.5 * jax.random.uniform(key_of[4], (COMPS, NBT, NODES), jnp.float32) ** level_of(key_of[4], (COMPS, NBT, NODES), ((1, 16),), -0.2, 0.2), 0.1, 0.6),
        "adjoint_end": noise(key_of[5], (COMPS, NBT, NODES), 1.0, 6.0, ((1, 16),), jnp.float32),
        "lift": noise(key_of[6], (FACES + 1, NODES, NODES), NODES ** -0.5, 0.5),
        "mixing": noise(key_of[7], (FACES + 1, COMPS, COMPS), (COMPS * (FACES + 1)) ** -0.5, 1.25, (), jnp.float32),
        "faces": with_ends(jax.random.randint(key_of[8], (NBT, FACES), 0, BLK_DEV + 4 * HALO), jax.random.fold_in(key_of[8], 1), 0, (BLK_DEV + 4 * HALO) - 1).astype(jnp.int32),
        "send_idx": with_ends(jax.random.randint(key_of[9], (N_SPACE, 4, HALO), 0, BLK_DEV), jax.random.fold_in(key_of[9], 1), 0, BLK_DEV - 1).astype(jnp.int32),
    }


OFFSETS = (1, -1, 2, -2)
STEP_SIZE = 0.5

def global_faces(faces, send_idx):
    total_blocks = faces.shape[0]
    blk_count = total_blocks // N_SPACE
    slot_count = send_idx.shape[2]
    owner_dev = (jnp.arange(total_blocks, dtype=jnp.int32) // blk_count)[:, None]
    inside = owner_dev * blk_count + faces
    beyond = jnp.maximum(faces - blk_count, 0)
    direction = beyond // slot_count
    slot_pos = beyond % slot_count
    shifts = jnp.array(OFFSETS, dtype=jnp.int32)[direction]
    source_dev = owner_dev - shifts
    is_valid = (source_dev >= 0) & (source_dev < N_SPACE)
    clipped = jnp.clip(source_dev, 0, N_SPACE - 1)
    flat_send = send_idx.reshape(-1)
    picked = flat_send[(clipped * 4 + direction) * slot_count + slot_pos]
    outside = jnp.where(is_valid, clipped * blk_count + picked, total_blocks)
    return jnp.where(faces < blk_count, inside, outside).astype(jnp.int32)

def residual_of(current, global_index, metric, lift_float, mixing):
    squashed = lax.optimization_barrier(jnp.tanh(current).astype(jnp.bfloat16))
    squashed = squashed.astype(jnp.float32)
    padded = jnp.concatenate([squashed, jnp.zeros((COMPS, 1, NODES), jnp.float32)], axis=1)
    totals = jnp.zeros(current.shape, jnp.float32)
    for face_slot in range(global_index.shape[1]):
        picked = padded[:, global_index[:, face_slot], :]
        products = jnp.einsum('cbj,ij->cbi', picked, lift_float[face_slot], precision=lax.Precision.HIGHEST)
        totals = totals + jnp.einsum('ec,cbi->ebi', mixing[face_slot], products, precision=lax.Precision.HIGHEST)
    return metric[None] * totals

def transpose_of(adjoint, current, global_index, metric, lift_float, mixing):
    total_blocks = current.shape[1]
    weighted = metric[None] * adjoint
    totals = jnp.zeros((COMPS, total_blocks + 1, NODES), jnp.float32)
    for face_slot in range(global_index.shape[1]):
        mixed = jnp.einsum('ec,ebi->cbi', mixing[face_slot], weighted, precision=lax.Precision.HIGHEST)
        mixed = lax.optimization_barrier(mixed.astype(jnp.bfloat16)).astype(jnp.float32)
        returned_terms = jnp.einsum('cbi,ij->cbj', mixed, lift_float[face_slot], precision=lax.Precision.HIGHEST)
        totals = totals.at[:, global_index[:, face_slot], :].add(returned_terms)
    derivative = 1.0 - jnp.tanh(current) ** 2
    return totals[:, :total_blocks, :] * derivative

def reference(checkpoints, sources, pitch, metric, obj_weight, adjoint_end, lift, mixing, faces, send_idx):
    total_blocks = faces.shape[0]
    own_index = jnp.arange(total_blocks, dtype=jnp.int32)[:, None]
    global_index = jnp.concatenate([own_index, global_faces(faces, send_idx)], axis=1).astype(jnp.int32)
    half_count = LEVELS // N_TM
    lift_float = lift.astype(jnp.float32)
    states = []
    current = checkpoints[0]
    for segment in range(N_TM):
        current = checkpoints[segment]
        for within in range(half_count):
            level_now = segment * half_count + within
            states.append(current)
            forcing = jnp.cos(pitch[level_now]) * sources[0] + jnp.sin(pitch[level_now]) * sources[1]
            current = current + STEP_SIZE * (forcing - residual_of(current, global_index, metric, lift_float, mixing))
    states.append(current)
    normalizer = math.sqrt(COMPS * NODES * total_blocks)
    adjoint = adjoint_end + obj_weight * states[LEVELS]
    grads = [None] * LEVELS
    bounds = [None, None]
    for level_now in reversed(range(LEVELS)):
        turning = jnp.cos(pitch[level_now]) * sources[1] - jnp.sin(pitch[level_now]) * sources[0]
        grads[level_now] = STEP_SIZE * jnp.sum(adjoint * turning) / normalizer
        adjoint = adjoint - STEP_SIZE * transpose_of(adjoint, states[level_now], global_index, metric, lift_float, mixing)
        if level_now > 0:
            adjoint = adjoint + obj_weight * states[level_now]
        if level_now % half_count == 0:
            bounds[level_now // half_count] = adjoint
    return (jnp.stack(bounds), jnp.stack(grads))
```

```python
import functools
import math

import jax
import jax.numpy as jnp
from jax import lax
from jax.experimental import pallas as pl
from jax.experimental.pallas import tpu as pltpu
from jax.sharding import PartitionSpec as P

OFFSETS = (1, -1, 2, -2)
STEP_SIZE = 0.5
F32 = jnp.float32
BF16 = jnp.bfloat16
MESH = pl.DeviceIdType.MESH


def dot(a, b):
    return jnp.dot(a, b, preferred_element_type=F32)


def window_kernel(
    dims,
    pitch_ref, mixing_ref, cp_hbm, src_hbm, metric_hbm, weight_hbm, end_hbm, lift_hbm, faces_hbm, send_hbm,
    out_ref, grad_ref,
    u_ref, lift_ref, faces_ref, send_ref, src_ref, metric_ref, weight_ref, a_ref, hand_ref, base_ref, dd_ref, wu_ref, lift_t, sq_ref,
    p_own, p_halo, pt_own, pt_halo, pick, pick_t, out_buf, in_buf, back_out, back_in, y_ref, yh_ref, z_ref,
    mixed_ref, g_ref, gw_ref, gh_ref, row_ref, rows_ref,
    pick_t2, low_ref, wf_ref, et_out, et_in, mg_out, mg_in, dup_out, dup_in, last_ref,
    load_sems, send_sems, recv_sems, bsend_sems, brecv_sems, hand_sems, factor_sems, gsend_sems, grecv_sems,
    table_sems, metric_sems, ghost_sems, dsend_sems, drecv_sems,
):
    comps, blocks, nodes, slots, halo, half, n_tm, n_space, norm = dims
    ghosts = 4 * halo
    faces_n = slots - 1
    wide = comps * nodes
    tm = lax.axis_index("tm")
    sp = lax.axis_index("space")
    n_dev = n_tm * n_space
    me = tm * n_space + sp
    lead = tm == n_tm - 1
    partner = (n_tm - 1 - tm, sp)
    segment = tm
    levels = half * n_tm

    loads = [
        pltpu.make_async_copy(send_hbm, send_ref, load_sems.at[5]),
        pltpu.make_async_copy(faces_hbm, faces_ref, load_sems.at[6]),
        pltpu.make_async_copy(cp_hbm.at[0], u_ref, load_sems.at[0]),
        pltpu.make_async_copy(lift_hbm, lift_ref, load_sems.at[7]),
        pltpu.make_async_copy(src_hbm, src_ref, load_sems.at[1]),
        pltpu.make_async_copy(metric_hbm, metric_ref, load_sems.at[2]),
        pltpu.make_async_copy(weight_hbm, weight_ref, load_sems.at[3]),
        pltpu.make_async_copy(end_hbm, a_ref, load_sems.at[4]),
    ]
    for load in loads:
        load.start()

    in_buf[...] = jnp.zeros_like(in_buf)

    @pl.when(lead)
    def _():
        back_in[...] = jnp.zeros_like(back_in)
        et_in[...] = jnp.zeros_like(et_in)
        mg_in[...] = jnp.zeros_like(mg_in)
        dup_in[...] = jnp.zeros_like(dup_in)

    barrier = pltpu.get_barrier_semaphore()

    def greet(r, carry):
        other = lax.rem(me + r, n_dev)
        pl.semaphore_signal(
            barrier, inc=1, device_id=(other // n_space, lax.rem(other, n_space)), device_id_type=MESH
        )
        return carry

    lax.fori_loop(1, n_dev, greet, 0)

    for load in loads[:2]:
        load.wait()
    row_ids = lax.broadcasted_iota(jnp.int32, (blocks, blocks), 0)
    lane_ids = lax.broadcasted_iota(jnp.int32, (blocks, blocks), 1)
    face_cols = []
    for k in range(faces_n):
        turned = jnp.broadcast_to(faces_ref[k : k + 1, :], (blocks, blocks))
        col = jnp.transpose(turned.astype(F32)).astype(jnp.int32)
        face_cols.append(col)
        p_own[k * blocks : (k + 1) * blocks, :] = (col == lane_ids).astype(F32).astype(BF16)
        pt_own[k * blocks : (k + 1) * blocks, :] = (turned == row_ids).astype(F32).astype(BF16)
        hit = (turned[:ghosts] == row_ids[:ghosts] + blocks).astype(F32).astype(BF16)
        pt_halo[k * ghosts : (k + 1) * ghosts, :blocks] = hit
        pt_halo[k * ghosts : (k + 1) * ghosts, blocks:] = hit
    for pair in range(faces_n // 2):
        low = lane_ids < ghosts
        col = jnp.where(low, face_cols[2 * pair], face_cols[2 * pair + 1])
        want = jnp.where(low, lane_ids, lane_ids - ghosts) + blocks
        p_halo[:, pair * 2 * ghosts : (pair + 1) * 2 * ghosts] = (col == want).astype(F32).astype(BF16)
    wanted = jnp.concatenate(
        [send_ref[0, d : d + 1, :] for d in range(4)] + [jnp.full((1, blocks - ghosts), -1, jnp.int32)], axis=1
    )
    spread = jnp.broadcast_to(wanted, (blocks, blocks))
    pick_t[...] = (spread == row_ids).astype(F32).astype(BF16)[:, :ghosts]
    doubled = jnp.concatenate([wanted[:, :ghosts]] * 2, axis=1)
    pick_t2[...] = (jnp.broadcast_to(doubled, (blocks, 2 * ghosts)) == row_ids).astype(F32).astype(BF16)
    spread_t = jnp.transpose(spread.astype(F32)).astype(jnp.int32)
    pick[...] = (spread_t[:ghosts] == lane_ids[:ghosts]).astype(F32).astype(BF16)
    row_ref[...] = jnp.zeros_like(row_ref)
    loads[2].wait()

    def lanes(c):
        return slice(c * nodes, (c + 1) * nodes)

    def target(shift):
        return (tm, jnp.clip(sp + shift, 0, n_space - 1))

    def inside(shift):
        return (sp + shift >= 0) & (sp + shift < n_space)

    def forward_copy(n, d):
        rows = pl.ds(d * halo, halo)
        return pltpu.make_async_remote_copy(
            src_ref=out_buf.at[n, rows], dst_ref=in_buf.at[segment * half + n, rows],
            send_sem=send_sems.at[n, d], recv_sem=recv_sems.at[n, d],
            device_id=target(OFFSETS[d]), device_id_type=MESH,
        )

    def ghost_copy(n, d):
        rows = pl.ds(d * halo, halo)
        return pltpu.make_async_remote_copy(
            src_ref=out_buf.at[n, rows], dst_ref=in_buf.at[n, rows],
            send_sem=ghost_sems.at[0, n // 2, d], recv_sem=ghost_sems.at[1, n // 2, d],
            device_id=(n_tm - 1, jnp.clip(sp + OFFSETS[d], 0, n_space - 1)), device_id_type=MESH,
        )

    def metric_copy(d):
        rows = pl.ds(d * halo, halo)
        return pltpu.make_async_remote_copy(
            src_ref=mg_out.at[rows], dst_ref=mg_in.at[rows],
            send_sem=metric_sems.at[0, d], recv_sem=metric_sems.at[1, d],
            device_id=target(OFFSETS[d]), device_id_type=MESH,
        )

    def table_copy(d):
        rows = pl.ds(d * faces_n * halo, faces_n * halo)
        return pltpu.make_async_remote_copy(
            src_ref=et_out.at[rows], dst_ref=et_in.at[rows],
            send_sem=table_sems.at[0, d], recv_sem=table_sems.at[1, d],
            device_id=target(-OFFSETS[d]), device_id_type=MESH,
        )

    def second_copy(slot, d, far):
        rows = pl.ds(far * halo, halo)
        return pltpu.make_async_remote_copy(
            src_ref=dup_out.at[slot, rows], dst_ref=dup_in.at[slot, d, rows],
            send_sem=dsend_sems.at[slot, 4 * d + far], recv_sem=drecv_sems.at[slot, 4 * d + far],
            device_id=target(-OFFSETS[far] - OFFSETS[d]), device_id_type=MESH,
        )

    def second_pairs():
        return [(d, far) for d in range(4) for far in range(4) if OFFSETS[d] + OFFSETS[far] != 0]

    def backward_copy(n, d):
        rows = pl.ds(d * halo, halo)
        return pltpu.make_async_remote_copy(
            src_ref=back_out.at[n, rows], dst_ref=back_in.at[n, rows],
            send_sem=bsend_sems.at[n, d], recv_sem=brecv_sems.at[n, d],
            device_id=target(-OFFSETS[d]), device_id_type=MESH,
        )

    def coef(k, e, c):
        return mixing_ref[k, e, c]

    def turn_of(level):
        angle = jnp.full((8, nodes), pitch_ref[level], F32)
        return jnp.cos(angle)[0:1], jnp.sin(angle)[0:1]

    for c in range(comps):
        sq_ref[:, lanes(c)] = jnp.tanh(u_ref[c]).astype(BF16)
    out_buf[0] = dot(pick[...], sq_ref[...]).astype(BF16)
    pl.semaphore_wait(barrier, n_dev - 1)
    for d in range(4):
        @pl.when(inside(OFFSETS[d]))
        def _():
            forward_copy(0, d).start()

    chunk = 32
    for load in loads[3:]:
        load.wait()
    for k in range(slots):
        lift_t[:, k * nodes : (k + 1) * nodes] = jnp.transpose(lift_ref[k].astype(F32)).astype(BF16)

    @pl.when(lead)
    def _():
        four = jnp.concatenate([wanted[:, :ghosts]] * 4, axis=1)
        ids = lax.broadcasted_iota(jnp.int32, (blocks, 4 * ghosts), 0)
        picks = (jnp.broadcast_to(four, (blocks, 4 * ghosts)) == ids).astype(F32).astype(BF16)
        table = dot(pt_halo[:, :blocks], picks)
        part = lax.broadcasted_iota(jnp.int32, (halo, 4 * ghosts), 1) // ghosts
        for d in range(4):
            for k in range(faces_n):
                piece = table[k * ghosts + d * halo : k * ghosts + (d + 1) * halo]
                to = (d * faces_n + k) * halo
                et_out[to : to + halo, :] = jnp.where(part == d, piece, 0.0).astype(BF16)
        mg_out[...] = dot(pick[...], metric_ref[...].astype(BF16)).astype(BF16)
        for d in range(4):
            @pl.when(inside(OFFSETS[d]))
            def _():
                metric_copy(d).start()

            @pl.when(inside(-OFFSETS[d]))
            def _():
                table_copy(d).start()

    def factor_copy(level, which):
        ref = (dd_ref, wu_ref)[which]
        return pltpu.make_async_remote_copy(
            src_ref=ref.at[level], dst_ref=ref.at[level], send_sem=factor_sems.at[0, which, level],
            recv_sem=factor_sems.at[1, which, level], device_id=partner, device_id_type=MESH,
        )

    def forward(n, carry):
        level = segment * half + n
        active = (n < half - 1) | lead

        @pl.when(n > 0)
        def _():
            for c in range(comps):
                sq_ref[:, lanes(c)] = jnp.tanh(u_ref[c]).astype(BF16)
            out_buf[n] = dot(pick[...], sq_ref[...]).astype(BF16)
            for d in range(4):
                @pl.when(inside(OFFSETS[d]) & active)
                def _():
                    forward_copy(n, d).start()

                @pl.when(inside(OFFSETS[d]) & jnp.logical_not(lead) & (lax.rem(n, 2) == 1))
                def _():
                    ghost_copy(n, d).start()

        keep = jnp.where(level > 0, 1.0, 0.0).astype(F32)
        for c in range(comps):
            state = u_ref[c]
            t = jnp.tanh(state)
            dd_ref[level, c] = STEP_SIZE * (1.0 - t * t)
            wu_ref[level, c] = (keep * weight_ref[c]) * state

        @pl.when(jnp.logical_not(lead))
        def _():
            factor_copy(level, 0).start()
            factor_copy(level, 1).start()

        @pl.when(active)
        def _():
            cosine, sine = turn_of(level)
            squashed = sq_ref[...]
            for k in range(slots):
                if k == 0:
                    got = squashed
                else:
                    got = dot(p_own[(k - 1) * blocks : k * blocks, :], squashed).astype(BF16)
                stacked = jnp.concatenate([got[:, lanes(c)] for c in range(comps)], axis=0)
                y_ref[k] = dot(stacked, lift_t[:, lanes(k)])

            def own_mix(r, carry):
                start = pl.multiple_of(r * chunk, chunk)
                metric_half = STEP_SIZE * metric_ref[pl.ds(start, chunk), :]
                sums = [None] * comps
                for k in range(slots):
                    for c in range(comps):
                        term = y_ref[k, pl.ds(c * blocks + start, chunk), :]
                        for e in range(comps):
                            add = coef(k, e, c) * term
                            sums[e] = add if sums[e] is None else sums[e] + add
                for e in range(comps):
                    rows = pl.ds(start, chunk)
                    forcing = cosine * src_ref[0, e, rows, :] + sine * src_ref[1, e, rows, :]
                    base_ref[e, rows, :] = u_ref[e, rows, :] + STEP_SIZE * forcing - metric_half * sums[e]
                return carry

            lax.fori_loop(0, blocks // chunk, own_mix, 0)

            for d in range(4):
                @pl.when(inside(-OFFSETS[d]))
                def _():
                    forward_copy(n, d).wait_recv()

            ghost = in_buf[level]
            stacked = jnp.concatenate([ghost[:, lanes(c)] for c in range(comps)], axis=0)
            yh_ref[...] = dot(stacked, lift_t[:, nodes:])
            for k in range(1, slots):
                for part in range(ghosts // chunk):
                    for e in range(comps):
                        total = None
                        for c in range(comps):
                            at = c * ghosts + part * chunk
                            add = coef(k, e, c) * yh_ref[at : at + chunk, lanes(k - 1)]
                            total = add if total is None else total + add
                        at = (k - 1) * ghosts + part * chunk
                        z_ref[at : at + chunk, lanes(e)] = total.astype(BF16)
            more = dot(p_halo[...], z_ref[...])
            half_metric = STEP_SIZE * metric_ref[...]
            for e in range(comps):
                u_ref[e] = base_ref[e] - half_metric * more[:, lanes(e)]
            for d in range(4):
                @pl.when(inside(OFFSETS[d]))
                def _():
                    forward_copy(n, d).wait_send()

        return carry

    lax.fori_loop(0, half, forward, 0)

    def hand_copy():
        return pltpu.make_async_remote_copy(
            src_ref=a_ref, dst_ref=out_ref.at[0], send_sem=hand_sems.at[0], recv_sem=hand_sems.at[1],
            device_id=partner, device_id_type=MESH,
        )

    def keep_copy():
        return pltpu.make_async_copy(hand_ref, out_ref.at[0], hand_sems.at[2])

    def grad_copy(source, other):
        return pltpu.make_async_remote_copy(
            src_ref=row_ref, dst_ref=rows_ref.at[source], send_sem=gsend_sems.at[other],
            recv_sem=grecv_sems.at[source], device_id=(other // n_space, lax.rem(other, n_space)),
            device_id_type=MESH,
        )

    def mix_back(k, at, rows, to):
        for c in range(comps):
            total = None
            for e in range(comps):
                add = coef(k, e, c) * gw_ref[at : at + rows, lanes(e)]
                total = add if total is None else total + add
            gh_ref[c * ghosts + to : c * ghosts + to + rows, lanes(k - 1)] = total.astype(BF16)

    def lift_back():
        return dot(gh_ref[...], lift_ref[1:].reshape(faces_n * nodes, nodes))

    def halo_part(ref, level, keep):
        for e in range(comps):
            w = metric_ref[...] * ref[e]
            if keep:
                wf_ref[e] = w
            high = w.astype(BF16)
            sq_ref[:, lanes(e)] = high
            low_ref[:, lanes(e)] = (w - high.astype(F32)).astype(BF16)
        gw_ref[...] = dot(pt_halo[...], jnp.concatenate([sq_ref[...], low_ref[...]], axis=0))
        for k in range(1, slots):
            for part in range(ghosts // chunk):
                mix_back(k, (k - 1) * ghosts + part * chunk, chunk, part * chunk)
        lifted = lift_back().astype(BF16)
        for c in range(comps):
            back_out[level, :, lanes(c)] = lifted[c * ghosts : (c + 1) * ghosts]
        for d in range(4):
            @pl.when(inside(-OFFSETS[d]))
            def _():
                backward_copy(level, d).start()

    def own_part(level):
        for k in range(slots):
            for r in range(blocks // chunk):
                rows = slice(r * chunk, (r + 1) * chunk)
                weighted = [wf_ref[e, rows, :] for e in range(comps)]
                for c in range(comps):
                    total = None
                    for e in range(comps):
                        add = coef(k, e, c) * weighted[e]
                        total = add if total is None else total + add
                    mixed_ref[k, rows, lanes(c)] = total.astype(BF16)
            if k == 0:
                got = mixed_ref[0]
            else:
                got = dot(pt_own[(k - 1) * blocks : k * blocks, :], mixed_ref[k]).astype(BF16)
            for c in range(comps):
                g_ref[c * blocks : (c + 1) * blocks, lanes(k)] = got[:, lanes(c)]
        pushed = dot(g_ref[...], lift_ref[...].reshape(slots * nodes, nodes))
        for c in range(comps):
            base_ref[c] = a_ref[c] + wu_ref[level, c] - dd_ref[level, c] * pushed[c * blocks : (c + 1) * blocks]

    def add_grad(level):
        cosine, sine = turn_of(level)
        sums = None
        for e in range(comps):
            part = a_ref[e] * (cosine * src_ref[1, e] - sine * src_ref[0, e])
            sums = part if sums is None else sums + part
        value = jnp.sum(jnp.sum(sums, axis=0, keepdims=True), axis=1, keepdims=True) * (STEP_SIZE / norm)
        spots = lax.broadcasted_iota(jnp.int32, (1, nodes), 1)
        row_ref[...] = row_ref[...] + jnp.where(spots == level, value, 0.0)

    def backward(j, carry):
        high = levels - 1 - 2 * j
        low = high - 1

        halo_part(a_ref, high, True)

        @pl.when(j == 0)
        def _():
            for d in range(4):
                @pl.when(inside(-OFFSETS[d]))
                def _():
                    metric_copy(d).wait_recv()

        @pl.when(high < half)
        def _():
            for d in range(4):
                @pl.when(inside(-OFFSETS[d]))
                def _():
                    ghost_copy(high, d).wait_recv()

            for which in range(2):
                factor_copy(high, which).wait_recv()
                factor_copy(low, which).wait_recv()

        spread_metric = mg_in[...].astype(F32)
        for c in range(comps):
            t = in_buf[high, :, lanes(c)].astype(F32)
            factor = spread_metric * (STEP_SIZE - STEP_SIZE * t * t)
            dup_out[j, :, lanes(c)] = (factor * back_out[high, :, lanes(c)].astype(F32)).astype(BF16)
        for d, far in second_pairs():
            @pl.when(inside(-OFFSETS[far]) & inside(-OFFSETS[far] - OFFSETS[d]))
            def _():
                second_copy(j, d, far).start()
        for far in range(4):
            d = OFFSETS.index(-OFFSETS[far])
            dup_in[j, d, far * halo : (far + 1) * halo, :] = dup_out[j, far * halo : (far + 1) * halo, :]

        add_grad(high)
        own_part(high)
        halo_part(base_ref, low, False)

        for d in range(4):
            @pl.when(inside(OFFSETS[d]))
            def _():
                backward_copy(high, d).wait_recv()

        more = dot(pick_t[...], back_in[high])
        for c in range(comps):
            state = base_ref[c] - dd_ref[high, c] * more[:, lanes(c)]
            a_ref[c] = state
            wf_ref[c] = metric_ref[...] * state

        add_grad(low)

        @pl.when(low == 0)
        def _():
            def tell(r, carry):
                grad_copy(sp, lax.rem(me + r, n_dev)).start()
                return carry

            lax.fori_loop(1, n_dev, tell, 0)

        own_part(low)

        @pl.when(j == 0)
        def _():
            for d in range(4):
                @pl.when(inside(OFFSETS[d]))
                def _():
                    table_copy(d).wait_recv()
                    metric_copy(d).wait_send()

                @pl.when(inside(-OFFSETS[d]))
                def _():
                    table_copy(d).wait_send()

        for d, far in second_pairs():
            @pl.when(inside(OFFSETS[d]) & inside(OFFSETS[d] + OFFSETS[far]))
            def _():
                second_copy(j, d, far).wait_recv()

        gw_ref[...] = dot(et_in[...], dup_in[j].reshape(4 * ghosts, wide))
        for k in range(1, slots):
            for d in range(4):
                mix_back(k, (d * faces_n + k - 1) * halo, halo, d * halo)
        lifted = lift_back()
        for c in range(comps):
            last_ref[ghosts:, lanes(c)] = (-lifted[c * ghosts : (c + 1) * ghosts]).astype(BF16)

        for d, far in second_pairs():
            @pl.when(inside(-OFFSETS[far]) & inside(-OFFSETS[far] - OFFSETS[d]))
            def _():
                second_copy(j, d, far).wait_send()
        for d in range(4):
            @pl.when(inside(-OFFSETS[d]))
            def _():
                backward_copy(high, d).wait_send()
                backward_copy(low, d).wait_send()

        for d in range(4):
            @pl.when(inside(OFFSETS[d]))
            def _():
                backward_copy(low, d).wait_recv()

        last_ref[:ghosts, :] = back_in[low]
        more = dot(pick_t2[...], last_ref[...])
        for c in range(comps):
            a_ref[c] = base_ref[c] - dd_ref[low, c] * more[:, lanes(c)]

        @pl.when(low == half)
        def _():
            for c in range(comps):
                hand_ref[c] = a_ref[c]
            keep_copy().start()

        return carry

    @pl.when(lead)
    def _():
        for c in range(comps):
            a_ref[c] = a_ref[c] + weight_ref[c] * u_ref[c]
        lax.fori_loop(0, levels // 2, backward, 0)
        hand_copy().start()
        rows_ref[sp] = row_ref[...]

        def settle(r, carry):
            other = lax.rem(sp + r, n_space)
            grad_copy(other, me).wait_recv()
            return carry

        lax.fori_loop(1, n_space, settle, 0)

    @pl.when(jnp.logical_not(lead))
    def _():
        def settle(r, carry):
            grad_copy(r, me).wait_recv()
            return carry

        lax.fori_loop(0, n_space, settle, 0)

    grad_ref[...] = jnp.sum(rows_ref[...], axis=0)[0, : grad_ref.shape[0]]

    @pl.when(lead)
    def _():
        hand_copy().wait_send()
        keep_copy().wait()

        def sent(r, carry):
            grad_copy(sp, lax.rem(me + r, n_dev)).wait_send()
            return carry

        lax.fori_loop(1, n_dev, sent, 0)

    @pl.when(jnp.logical_not(lead))
    def _():
        hand_copy().wait_recv()
        for level in range(half):
            factor_copy(level, 0).wait_send()
            factor_copy(level, 1).wait_send()
        for level in range(1, half, 2):
            for d in range(4):
                @pl.when(inside(OFFSETS[d]))
                def _():
                    ghost_copy(level, d).wait_send()


def shards(
    checkpoints, sources, pitch, metric, obj_weight, adjoint_end, lift, mixing, faces, send_idx
):
    comps = sources.shape[1]
    blocks, nodes = metric.shape
    slots = lift.shape[0]
    halo = send_idx.shape[2]
    n_tm = lax.axis_size("tm")
    n_space = lax.axis_size("space")
    levels = pitch.shape[0]
    half = levels // n_tm
    ghosts = 4 * halo
    norm = math.sqrt(comps * nodes * blocks * n_space)
    wide = comps * nodes
    field = (comps, blocks, nodes)
    vmem = pl.BlockSpec(memory_space=pltpu.VMEM)
    smem = pl.BlockSpec(memory_space=pltpu.SMEM)
    anym = pl.BlockSpec(memory_space=pl.ANY)
    dma = pltpu.SemaphoreType.DMA
    n_dev = n_tm * n_space
    dims = (comps, blocks, nodes, slots, halo, half, n_tm, n_space, norm)
    bounds, grad = pl.pallas_call(
        functools.partial(window_kernel, dims),
        out_shape=(
            jax.ShapeDtypeStruct((1, *field), F32),
            jax.ShapeDtypeStruct((levels,), F32),
        ),
        in_specs=[smem, smem] + [anym] * 8,
        out_specs=(anym, vmem),
        scratch_shapes=[
            pltpu.VMEM(field, F32),
            pltpu.VMEM(lift.shape, BF16),
            pltpu.VMEM(faces.shape[::-1], jnp.int32),
            pltpu.VMEM(send_idx.shape, jnp.int32),
            pltpu.VMEM((2, *field), F32),
            pltpu.VMEM((blocks, nodes), F32),
            pltpu.VMEM(field, F32),
            pltpu.VMEM(field, F32),
            pltpu.VMEM(field, F32),
            pltpu.VMEM(field, F32),
            pltpu.VMEM((levels, *field), F32),
            pltpu.VMEM((levels, *field), F32),
            pltpu.VMEM((nodes, slots * nodes), BF16),
            pltpu.VMEM((blocks, wide), BF16),
            pltpu.VMEM(((slots - 1) * blocks, blocks), BF16),
            pltpu.VMEM((blocks, (slots - 1) * ghosts), BF16),
            pltpu.VMEM(((slots - 1) * blocks, blocks), BF16),
            pltpu.VMEM(((slots - 1) * ghosts, 2 * blocks), BF16),
            pltpu.VMEM((ghosts, blocks), BF16),
            pltpu.VMEM((blocks, ghosts), BF16),
            pltpu.VMEM((half, ghosts, wide), BF16),
            pltpu.VMEM((levels, ghosts, wide), BF16),
            pltpu.VMEM((levels, ghosts, wide), BF16),
            pltpu.VMEM((levels, ghosts, wide), BF16),
            pltpu.VMEM((slots, comps * blocks, nodes), F32),
            pltpu.VMEM((comps * ghosts, (slots - 1) * nodes), F32),
            pltpu.VMEM(((slots - 1) * ghosts, wide), BF16),
            pltpu.VMEM((slots, blocks, wide), BF16),
            pltpu.VMEM((comps * blocks, slots * nodes), BF16),
            pltpu.VMEM(((slots - 1) * ghosts, wide), F32),
            pltpu.VMEM((comps * ghosts, (slots - 1) * nodes), BF16),
            pltpu.VMEM((1, nodes), F32),
            pltpu.VMEM((n_space, 1, nodes), F32),
            pltpu.VMEM((blocks, 2 * ghosts), BF16),
            pltpu.VMEM((blocks, wide), BF16),
            pltpu.VMEM(field, F32),
            pltpu.VMEM(((slots - 1) * ghosts, 4 * ghosts), BF16),
            pltpu.VMEM(((slots - 1) * ghosts, 4 * ghosts), BF16),
            pltpu.VMEM((ghosts, nodes), BF16),
            pltpu.VMEM((ghosts, nodes), BF16),
            pltpu.VMEM((levels // 2, ghosts, wide), BF16),
            pltpu.VMEM((levels // 2, 4, ghosts, wide), BF16),
            pltpu.VMEM((2 * ghosts, wide), BF16),
            dma((8,)),
            dma((half, 4)),
            dma((half, 4)),
            dma((levels, 4)),
            dma((levels, 4)),
            dma((3,)),
            dma((2, 2, half)),
            dma((n_dev,)),
            dma((n_space,)),
            dma((2, 4)),
            dma((2, 4)),
            dma((2, half // 2, 4)),
            dma((levels // 2, 16)),
            dma((levels // 2, 16)),
        ],
        compiler_params=pltpu.CompilerParams(
            collective_id=0, has_side_effects=True, vmem_limit_bytes=60 * 1024 * 1024
        ),
        name="window",
    )(pitch, mixing, checkpoints, sources, metric, obj_weight, adjoint_end, lift, faces.T, send_idx)
    return bounds, grad


def solution(mesh):
    placed = (
        P("tm", None, "space", None),
        P(None, None, "space", None),
        P(),
        P("space", None),
        P(None, "space", None),
        P(None, "space", None),
        P(),
        P(),
        P("space", None),
        P("space", None, None),
    )
    return jax.shard_map(
        shards,
        mesh=mesh,
        in_specs=placed,
        out_specs=(P("tm", None, "space", None), P()),
        check_vma=False,
    )
```

```python
import functools
import math

import jax
import jax.numpy as jnp
from jax import lax
from jax.experimental import pallas as pl
from jax.experimental.pallas import tpu as pltpu
from jax.sharding import PartitionSpec as P

OFFSETS = (1, -1, 2, -2)
STEP_SIZE = 0.5
F32 = jnp.float32
BF16 = jnp.bfloat16
MESH = pl.DeviceIdType.MESH
DIRS = range(4)


def dot(a, b):
    return jnp.dot(a, b, preferred_element_type=F32)


def one_hot(hit):
    return hit.astype(F32).astype(BF16)


def beside(parts):
    return jnp.concatenate(list(parts), axis=1)


def below(parts):
    return jnp.concatenate(list(parts), axis=0)


def rounds_of(n_space):
    reach, rounds = 2 * max(OFFSETS), []
    while reach < n_space - 1:
        rounds.append(reach)
        reach *= 2
    return rounds


def window_kernel(
    dims,
    pitch_hbm, mixing_hbm, cp_hbm, src_hbm, metric_hbm, weight_hbm, end_hbm, lift_hbm, faces_hbm, send_hbm,
    out_ref, grad_ref,
    pitch_ref, mixing_ref, u_ref, lift_ref, faces_ref, send_ref, src_ref, metric_ref, weight_ref, a_ref, hand_ref,
    base_ref, dd_ref, wu_ref, lift_t, sq_ref,
    p_own, p_halo, pt_own, pt_halo, pick, pick_t, pick_t2, out_buf, in_buf, back_out, back_in, y_ref, yh_ref, z_ref,
    mixed_ref, g_ref, gw_ref, gh_ref, split_ref, wf_ref, row_ref, rows_ref,
    et_out, et_in, mg_out, mg_in, dup_out, dup_in, last_ref,
    load_sems, send_sems, recv_sems, bsend_sems, brecv_sems, hand_sems, factor_sems, gsend_sems, grecv_sems,
    table_sems, metric_sems, ghost_sems, dsend_sems, drecv_sems, round_sems,
):
    comps, blocks, nodes, slots, halo, half, n_tm, n_space, norm = dims
    ghosts = 4 * halo
    faces_n = slots - 1
    tm = lax.axis_index("tm")
    sp = lax.axis_index("space")
    n_dev = n_tm * n_space
    me = tm * n_space + sp
    lead = tm == n_tm - 1
    partner = (n_tm - 1 - tm, sp)
    levels = half * n_tm
    rounds = rounds_of(n_space)
    chunk = 32

    pairs = [
        (send_hbm, send_ref),
        (cp_hbm.at[0], u_ref),
        (faces_hbm, faces_ref),
        (pitch_hbm, pitch_ref),
        (mixing_hbm, mixing_ref),
        (lift_hbm, lift_ref),
        (metric_hbm, metric_ref),
        (weight_hbm, weight_ref),
        (src_hbm, src_ref),
        (end_hbm, a_ref),
    ]
    loads = [pltpu.make_async_copy(src, dst, load_sems.at[i]) for i, (src, dst) in enumerate(pairs)]
    for load in loads:
        load.start()

    in_buf[...] = jnp.zeros_like(in_buf)

    @pl.when(lead)
    def _():
        et_in[...] = jnp.zeros_like(et_in)
        mg_in[...] = jnp.zeros_like(mg_in)

    barrier = pltpu.get_barrier_semaphore()

    def inside(shift):
        return (sp + shift >= 0) & (sp + shift < n_space)

    def at(shift):
        return jnp.clip(sp + shift, 0, n_space - 1)

    met = n_tm - 1
    pl.semaphore_signal(barrier, inc=1, device_id=partner, device_id_type=MESH)
    for shift in OFFSETS:
        met = met + n_tm * inside(shift).astype(jnp.int32)

        @pl.when(inside(shift))
        def _():
            for side in range(n_tm):
                pl.semaphore_signal(barrier, inc=1, device_id=(side, at(shift)), device_id_type=MESH)

    def lanes(c):
        return slice(c * nodes, (c + 1) * nodes)

    def target(shift):
        return (tm, at(shift))

    def forward_copy(n, d):
        return pltpu.make_async_remote_copy(
            src_ref=out_buf.at[n, d], dst_ref=in_buf.at[tm * half + n, d],
            send_sem=send_sems.at[n, d], recv_sem=recv_sems.at[n, d],
            device_id=target(OFFSETS[d]), device_id_type=MESH,
        )

    def ghost_copy(n, d):
        return pltpu.make_async_remote_copy(
            src_ref=out_buf.at[n, d], dst_ref=in_buf.at[n, d],
            send_sem=ghost_sems.at[0, n // 2, d], recv_sem=ghost_sems.at[1, n // 2, d],
            device_id=(n_tm - 1, at(OFFSETS[d])), device_id_type=MESH,
        )

    def metric_copy(d):
        return pltpu.make_async_remote_copy(
            src_ref=mg_out.at[d], dst_ref=mg_in.at[d],
            send_sem=metric_sems.at[0, d], recv_sem=metric_sems.at[1, d],
            device_id=target(OFFSETS[d]), device_id_type=MESH,
        )

    def table_copy(d):
        rows = pl.ds(d * faces_n * halo, faces_n * halo)
        return pltpu.make_async_remote_copy(
            src_ref=et_out.at[rows], dst_ref=et_in.at[rows],
            send_sem=table_sems.at[0, d], recv_sem=table_sems.at[1, d],
            device_id=target(-OFFSETS[d]), device_id_type=MESH,
        )

    def second_copy(slot, d, far):
        return pltpu.make_async_remote_copy(
            src_ref=dup_out.at[slot, far], dst_ref=dup_in.at[slot, d, far],
            send_sem=dsend_sems.at[slot, 4 * d + far], recv_sem=drecv_sems.at[slot, 4 * d + far],
            device_id=target(-OFFSETS[far] - OFFSETS[d]), device_id_type=MESH,
        )

    second_pairs = [(d, far) for d in DIRS for far in DIRS if OFFSETS[d] + OFFSETS[far] != 0]
    second_pairs = sorted(second_pairs, key=lambda p: -abs(OFFSETS[p[0]] + OFFSETS[p[1]]))

    def backward_copy(n, d):
        return pltpu.make_async_remote_copy(
            src_ref=back_out.at[n, d], dst_ref=back_in.at[n, d],
            send_sem=bsend_sems.at[n, d], recv_sem=brecv_sems.at[n, d],
            device_id=target(-OFFSETS[d]), device_id_type=MESH,
        )

    def coef(k, e, c):
        return mixing_ref[k, e, c]

    def turn_of(level):
        angle = jnp.full((8, nodes), pitch_ref[level], F32)
        return jnp.cos(angle)[0:1], jnp.sin(angle)[0:1]

    def ghost_rows(ref, index, c):
        return below(ref[index + (d, c)] for d in DIRS)

    def ghost_wide(ref, index):
        return beside(ghost_rows(ref, index, c) for c in range(comps))

    def squash_and_pick(n):
        for c in range(comps):
            sq_ref[c] = jnp.tanh(u_ref[c]).astype(BF16)
        picked = dot(pick[...], beside(sq_ref[c] for c in range(comps))).astype(BF16)
        for d in DIRS:
            for c in range(comps):
                out_buf[n, d, c] = picked[d * halo : (d + 1) * halo, lanes(c)]

    row_ids = lax.broadcasted_iota(jnp.int32, (blocks, blocks), 0)
    lane_ids = lax.broadcasted_iota(jnp.int32, (blocks, blocks), 1)
    loads[0].wait()
    wanted = beside(
        [send_ref[0, d : d + 1, :] for d in DIRS] + [jnp.full((1, blocks - ghosts), -1, jnp.int32)]
    )
    spread = jnp.broadcast_to(wanted, (blocks, blocks))
    spread_t = jnp.transpose(spread.astype(F32)).astype(jnp.int32)
    pick[...] = one_hot(spread_t[:ghosts] == lane_ids[:ghosts])
    loads[1].wait()
    squash_and_pick(0)
    pl.semaphore_wait(barrier, met)
    for d in DIRS:
        @pl.when(inside(OFFSETS[d]))
        def _():
            forward_copy(0, d).start()

    pick_t[...] = one_hot(spread == row_ids)[:, :ghosts]
    doubled = beside([wanted[:, :ghosts]] * 2)
    pick_t2[...] = one_hot(jnp.broadcast_to(doubled, (blocks, 2 * ghosts)) == row_ids)
    row_ref[...] = jnp.zeros_like(row_ref)
    loads[2].wait()
    face_cols = []
    for k in range(faces_n):
        turned = jnp.broadcast_to(faces_ref[k : k + 1, :], (blocks, blocks))
        col = jnp.transpose(turned.astype(F32)).astype(jnp.int32)
        face_cols.append(col)
        p_own[k * blocks : (k + 1) * blocks, :] = one_hot(col == lane_ids)
        pt_own[k * blocks : (k + 1) * blocks, :] = one_hot(turned == row_ids)
        hit = one_hot(turned[:ghosts] == row_ids[:ghosts] + blocks)
        pt_halo[k * ghosts : (k + 1) * ghosts, :blocks] = hit
        pt_halo[k * ghosts : (k + 1) * ghosts, blocks:] = hit
    for pair in range(faces_n // 2):
        low = lane_ids < ghosts
        col = jnp.where(low, face_cols[2 * pair], face_cols[2 * pair + 1])
        want = jnp.where(low, lane_ids, lane_ids - ghosts) + blocks
        p_halo[:, pair * 2 * ghosts : (pair + 1) * 2 * ghosts] = one_hot(col == want)

    for load in loads[3:]:
        load.wait()
    for k in range(slots):
        lift_t[:, k * nodes : (k + 1) * nodes] = jnp.transpose(lift_ref[k].astype(F32)).astype(BF16)

    @pl.when(lead)
    def _():
        back_in[...] = jnp.zeros_like(back_in)
        dup_in[...] = jnp.zeros_like(dup_in)
        four = beside([wanted[:, :ghosts]] * 4)
        ids = lax.broadcasted_iota(jnp.int32, (blocks, 4 * ghosts), 0)
        picks = one_hot(jnp.broadcast_to(four, (blocks, 4 * ghosts)) == ids)
        table = dot(pt_halo[:, :blocks], picks)
        part = lax.broadcasted_iota(jnp.int32, (halo, 4 * ghosts), 1) // ghosts
        for d in DIRS:
            for k in range(faces_n):
                piece = table[k * ghosts + d * halo : k * ghosts + (d + 1) * halo]
                to = (d * faces_n + k) * halo
                et_out[to : to + halo, :] = jnp.where(part == d, piece, 0.0).astype(BF16)
        chosen = dot(pick[...], metric_ref[...].astype(BF16)).astype(BF16)
        for d in DIRS:
            mg_out[d] = chosen[d * halo : (d + 1) * halo]
        for d in DIRS:
            @pl.when(inside(OFFSETS[d]))
            def _():
                metric_copy(d).start()

            @pl.when(inside(-OFFSETS[d]))
            def _():
                table_copy(d).start()

    def factor_copy(level, which):
        ref = (dd_ref, wu_ref)[which]
        return pltpu.make_async_remote_copy(
            src_ref=ref.at[level], dst_ref=ref.at[level], send_sem=factor_sems.at[0, which, level],
            recv_sem=factor_sems.at[1, which, level], device_id=partner, device_id_type=MESH,
        )

    def round_signal(r):
        for side, shift in enumerate((rounds[r], -rounds[r])):
            @pl.when(inside(shift))
            def _():
                pl.semaphore_signal(
                    round_sems.at[r, side], inc=1, device_id=(n_tm - 1, at(shift)), device_id_type=MESH
                )

    def round_wait(r):
        for side, shift in enumerate((rounds[r], -rounds[r])):
            @pl.when(inside(-shift))
            def _():
                pl.semaphore_wait(round_sems.at[r, side], 1)

    def round_step(r):
        if 0 < r <= len(rounds):
            round_wait(r - 1)
        if r < len(rounds):
            round_signal(r)

    def forward(n, carry):
        level = tm * half + n
        active = (n < half - 1) | lead

        @pl.when(n > 0)
        def _():
            squash_and_pick(n)
            for d in DIRS:
                @pl.when(inside(OFFSETS[d]) & active)
                def _():
                    forward_copy(n, d).start()

                @pl.when(inside(OFFSETS[d]) & jnp.logical_not(lead) & (lax.rem(n, 2) == 1))
                def _():
                    ghost_copy(n, d).start()

        for r in range(half - 1):
            @pl.when(lead & (n == r + 1))
            def _():
                round_step(r)

        keep = jnp.where(level > 0, 1.0, 0.0).astype(F32)
        for c in range(comps):
            state = u_ref[c]
            t = jnp.tanh(state)
            dd_ref[level, c] = STEP_SIZE * (1.0 - t * t)
            wu_ref[level, c] = (keep * weight_ref[c]) * state

        @pl.when(jnp.logical_not(lead))
        def _():
            factor_copy(level, 0).start()
            factor_copy(level, 1).start()

        @pl.when(active)
        def _():
            cosine, sine = turn_of(level)
            squashed = beside(sq_ref[c] for c in range(comps))
            for k in range(slots):
                if k == 0:
                    stacked = sq_ref[...].reshape(comps * blocks, nodes)
                else:
                    got = dot(p_own[(k - 1) * blocks : k * blocks, :], squashed).astype(BF16)
                    stacked = below(got[:, lanes(c)] for c in range(comps))
                y_ref[k] = dot(stacked, lift_t[:, lanes(k)])

            def own_mix(r, carry):
                start = pl.multiple_of(r * chunk, chunk)
                metric_half = STEP_SIZE * metric_ref[pl.ds(start, chunk), :]
                sums = [None] * comps
                for k in range(slots):
                    for c in range(comps):
                        term = y_ref[k, pl.ds(c * blocks + start, chunk), :]
                        for e in range(comps):
                            add = coef(k, e, c) * term
                            sums[e] = add if sums[e] is None else sums[e] + add
                for e in range(comps):
                    rows = pl.ds(start, chunk)
                    forcing = cosine * src_ref[0, e, rows, :] + sine * src_ref[1, e, rows, :]
                    base_ref[e, rows, :] = u_ref[e, rows, :] + STEP_SIZE * forcing - metric_half * sums[e]
                return carry

            lax.fori_loop(0, blocks // chunk, own_mix, 0)

            for d in DIRS:
                @pl.when(inside(OFFSETS[d]))
                def _():
                    forward_copy(n, d).wait_send()

            for d in DIRS:
                @pl.when(inside(-OFFSETS[d]))
                def _():
                    forward_copy(n, d).wait_recv()

            stacked = below(ghost_rows(in_buf, (level,), c) for c in range(comps))
            yh_ref[...] = dot(stacked, lift_t[:, nodes:])
            for k in range(1, slots):
                for part in range(ghosts // chunk):
                    for e in range(comps):
                        total = None
                        for c in range(comps):
                            row = c * ghosts + part * chunk
                            add = coef(k, e, c) * yh_ref[row : row + chunk, lanes(k - 1)]
                            total = add if total is None else total + add
                        row = (k - 1) * ghosts + part * chunk
                        z_ref[e, row : row + chunk, :] = total.astype(BF16)
            more = dot(p_halo[...], beside(z_ref[e] for e in range(comps)))
            half_metric = STEP_SIZE * metric_ref[...]
            for e in range(comps):
                u_ref[e] = base_ref[e] - half_metric * more[:, lanes(e)]

        return carry

    lax.fori_loop(0, half, forward, 0)

    def hand_copy():
        return pltpu.make_async_remote_copy(
            src_ref=a_ref, dst_ref=out_ref.at[0], send_sem=hand_sems.at[0], recv_sem=hand_sems.at[1],
            device_id=partner, device_id_type=MESH,
        )

    def keep_copy():
        return pltpu.make_async_copy(hand_ref, out_ref.at[0], hand_sems.at[2])

    def grad_copy(source, other):
        return pltpu.make_async_remote_copy(
            src_ref=row_ref, dst_ref=rows_ref.at[source], send_sem=gsend_sems.at[other],
            recv_sem=grecv_sems.at[source], device_id=(other // n_space, lax.rem(other, n_space)),
            device_id_type=MESH,
        )

    def mix_back(k, row, rows, to):
        for c in range(comps):
            total = None
            for e in range(comps):
                add = coef(k, e, c) * gw_ref[row : row + rows, lanes(e)]
                total = add if total is None else total + add
            gh_ref[k - 1, c * ghosts + to : c * ghosts + to + rows, :] = total.astype(BF16)

    def lift_back():
        return dot(beside(gh_ref[k] for k in range(faces_n)), lift_ref[1:].reshape(faces_n * nodes, nodes))

    def halo_part(ref, level, keep):
        for e in range(comps):
            w = metric_ref[...] * ref[e]
            if keep:
                wf_ref[e] = w
            high = w.astype(BF16)
            split_ref[e, :blocks, :] = high
            split_ref[e, blocks:, :] = (w - high.astype(F32)).astype(BF16)
        gw_ref[...] = dot(pt_halo[...], beside(split_ref[e] for e in range(comps)))
        for k in range(1, slots):
            for part in range(ghosts // chunk):
                mix_back(k, (k - 1) * ghosts + part * chunk, chunk, part * chunk)
        lifted = lift_back().astype(BF16)
        for d in DIRS:
            for c in range(comps):
                row = c * ghosts + d * halo
                back_out[level, d, c] = lifted[row : row + halo]
        for d in DIRS:
            @pl.when(inside(-OFFSETS[d]))
            def _():
                backward_copy(level, d).start()

    def own_part(level):
        for k in range(slots):
            for r in range(blocks // chunk):
                rows = slice(r * chunk, (r + 1) * chunk)
                weighted = [wf_ref[e, rows, :] for e in range(comps)]
                for c in range(comps):
                    total = None
                    for e in range(comps):
                        add = coef(k, e, c) * weighted[e]
                        total = add if total is None else total + add
                    if k == 0:
                        g_ref[0, c * blocks + r * chunk : c * blocks + (r + 1) * chunk, :] = total.astype(BF16)
                    else:
                        mixed_ref[k - 1, c, rows, :] = total.astype(BF16)
            if k > 0:
                wide = beside(mixed_ref[k - 1, c] for c in range(comps))
                got = dot(pt_own[(k - 1) * blocks : k * blocks, :], wide).astype(BF16)
                for c in range(comps):
                    g_ref[k, c * blocks : (c + 1) * blocks, :] = got[:, lanes(c)]
        pushed = dot(beside(g_ref[k] for k in range(slots)), lift_ref[...].reshape(slots * nodes, nodes))
        for c in range(comps):
            base_ref[c] = a_ref[c] + wu_ref[level, c] - dd_ref[level, c] * pushed[c * blocks : (c + 1) * blocks]

    def add_grad(level):
        cosine, sine = turn_of(level)
        sums = None
        for e in range(comps):
            part = a_ref[e] * (cosine * src_ref[1, e] - sine * src_ref[0, e])
            sums = part if sums is None else sums + part
        value = jnp.sum(jnp.sum(sums, axis=0, keepdims=True), axis=1, keepdims=True) * (STEP_SIZE / norm)
        spots = lax.broadcasted_iota(jnp.int32, (1, nodes), 1)
        row_ref[...] = row_ref[...] + jnp.where(spots == level, value, 0.0)

    def backward(j, carry):
        high = levels - 1 - 2 * j
        low = high - 1

        halo_part(a_ref, high, True)

        @pl.when(j == 0)
        def _():
            for d in DIRS:
                @pl.when(inside(-OFFSETS[d]))
                def _():
                    metric_copy(d).wait_recv()

        @pl.when(high < half)
        def _():
            for d in DIRS:
                @pl.when(inside(-OFFSETS[d]))
                def _():
                    ghost_copy(high, d).wait_recv()

            for which in range(2):
                factor_copy(high, which).wait_recv()
                factor_copy(low, which).wait_recv()

        for far in DIRS:
            spread_metric = mg_in[far].astype(F32)
            d = OFFSETS.index(-OFFSETS[far])
            for c in range(comps):
                t = in_buf[high, far, c].astype(F32)
                factor = spread_metric * (STEP_SIZE - STEP_SIZE * t * t)
                scaled = (factor * back_out[high, far, c].astype(F32)).astype(BF16)
                dup_out[j, far, c] = scaled
                dup_in[j, d, far, c] = scaled
        for d, far in second_pairs:
            @pl.when(inside(-OFFSETS[far]) & inside(-OFFSETS[far] - OFFSETS[d]))
            def _():
                second_copy(j, d, far).start()

        own_part(high)
        halo_part(base_ref, low, False)
        add_grad(high)

        for d in DIRS:
            @pl.when(inside(OFFSETS[d]))
            def _():
                backward_copy(high, d).wait_recv()

        more = dot(pick_t[...], ghost_wide(back_in, (high,)))
        for c in range(comps):
            state = base_ref[c] - dd_ref[high, c] * more[:, lanes(c)]
            a_ref[c] = state
            wf_ref[c] = metric_ref[...] * state

        add_grad(low)

        @pl.when(low == 0)
        def _():
            def tell(r, carry):
                grad_copy(sp, lax.rem(me + r, n_dev)).start()
                return carry

            lax.fori_loop(1, n_dev, tell, 0)

        own_part(low)

        @pl.when(j == 0)
        def _():
            for d in DIRS:
                @pl.when(inside(OFFSETS[d]))
                def _():
                    table_copy(d).wait_recv()
                    metric_copy(d).wait_send()

                @pl.when(inside(-OFFSETS[d]))
                def _():
                    table_copy(d).wait_send()

        for d, far in second_pairs:
            @pl.when(inside(OFFSETS[d]) & inside(OFFSETS[d] + OFFSETS[far]))
            def _():
                second_copy(j, d, far).wait_recv()

        rows = [below(dup_in[j, d, far, c] for d in DIRS for far in DIRS) for c in range(comps)]
        gw_ref[...] = dot(et_in[...], beside(rows))
        for k in range(1, slots):
            for d in DIRS:
                mix_back(k, (d * faces_n + k - 1) * halo, halo, d * halo)
        lifted = (-lift_back()).astype(BF16)
        for c in range(comps):
            last_ref[c] = lifted[c * ghosts : (c + 1) * ghosts]

        for d, far in second_pairs:
            @pl.when(inside(-OFFSETS[far]) & inside(-OFFSETS[far] - OFFSETS[d]))
            def _():
                second_copy(j, d, far).wait_send()
        for d in DIRS:
            @pl.when(inside(-OFFSETS[d]))
            def _():
                backward_copy(high, d).wait_send()
                backward_copy(low, d).wait_send()

        for d in DIRS:
            @pl.when(inside(OFFSETS[d]))
            def _():
                backward_copy(low, d).wait_recv()

        late = beside(below([ghost_rows(back_in, (low,), c), last_ref[c]]) for c in range(comps))
        more = dot(pick_t2[...], late)
        for c in range(comps):
            a_ref[c] = base_ref[c] - dd_ref[low, c] * more[:, lanes(c)]

        @pl.when(low == half)
        def _():
            for c in range(comps):
                hand_ref[c] = a_ref[c]
            keep_copy().start()

        return carry

    @pl.when(lead)
    def _():
        for r in range(half - 1, len(rounds) + 1):
            round_step(r)
        for c in range(comps):
            a_ref[c] = a_ref[c] + weight_ref[c] * u_ref[c]
        lax.fori_loop(0, levels // 2, backward, 0)
        hand_copy().start()
        rows_ref[sp] = row_ref[...]

        def settle(r, carry):
            other = lax.rem(sp + r, n_space)
            grad_copy(other, me).wait_recv()
            return carry

        lax.fori_loop(1, n_space, settle, 0)

    @pl.when(jnp.logical_not(lead))
    def _():
        def settle(r, carry):
            grad_copy(r, me).wait_recv()
            return carry

        lax.fori_loop(0, n_space, settle, 0)

    grad_ref[...] = jnp.sum(rows_ref[...], axis=0)[0, : grad_ref.shape[0]]

    @pl.when(lead)
    def _():
        hand_copy().wait_send()
        keep_copy().wait()

        def sent(r, carry):
            grad_copy(sp, lax.rem(me + r, n_dev)).wait_send()
            return carry

        lax.fori_loop(1, n_dev, sent, 0)

    @pl.when(jnp.logical_not(lead))
    def _():
        hand_copy().wait_recv()
        for level in range(half):
            factor_copy(level, 0).wait_send()
            factor_copy(level, 1).wait_send()
        for level in range(1, half, 2):
            for d in DIRS:
                @pl.when(inside(OFFSETS[d]))
                def _():
                    ghost_copy(level, d).wait_send()


def shards(
    checkpoints, sources, pitch, metric, obj_weight, adjoint_end, lift, mixing, faces, send_idx
):
    comps = sources.shape[1]
    blocks, nodes = metric.shape
    slots = lift.shape[0]
    faces_n = slots - 1
    halo = send_idx.shape[2]
    n_tm = lax.axis_size("tm")
    n_space = lax.axis_size("space")
    levels = pitch.shape[0]
    half = levels // n_tm
    twos = levels // 2
    ghosts = 4 * halo
    norm = math.sqrt(comps * nodes * blocks * n_space)
    wide = comps * nodes
    field = (comps, blocks, nodes)
    group = (4, comps, halo, nodes)
    vmem = pl.BlockSpec(memory_space=pltpu.VMEM)
    anym = pl.BlockSpec(memory_space=pl.ANY)
    dma = pltpu.SemaphoreType.DMA
    n_dev = n_tm * n_space
    dims = (comps, blocks, nodes, slots, halo, half, n_tm, n_space, norm)
    bounds, grad = pl.pallas_call(
        functools.partial(window_kernel, dims),
        out_shape=(
            jax.ShapeDtypeStruct((1, *field), F32),
            jax.ShapeDtypeStruct((levels,), F32),
        ),
        in_specs=[anym] * 10,
        out_specs=(anym, vmem),
        scratch_shapes=[
            pltpu.SMEM(pitch.shape, F32),
            pltpu.SMEM(mixing.shape, F32),
            pltpu.VMEM(field, F32),
            pltpu.VMEM(lift.shape, BF16),
            pltpu.VMEM(faces.shape[::-1], jnp.int32),
            pltpu.VMEM(send_idx.shape, jnp.int32),
            pltpu.VMEM((2, *field), F32),
            pltpu.VMEM((blocks, nodes), F32),
            pltpu.VMEM(field, F32),
            pltpu.VMEM(field, F32),
            pltpu.VMEM(field, F32),
            pltpu.VMEM(field, F32),
            pltpu.VMEM((levels, *field), F32),
            pltpu.VMEM((levels, *field), F32),
            pltpu.VMEM((nodes, slots * nodes), BF16),
            pltpu.VMEM(field, BF16),
            pltpu.VMEM((faces_n * blocks, blocks), BF16),
            pltpu.VMEM((blocks, faces_n * ghosts), BF16),
            pltpu.VMEM((faces_n * blocks, blocks), BF16),
            pltpu.VMEM((faces_n * ghosts, 2 * blocks), BF16),
            pltpu.VMEM((ghosts, blocks), BF16),
            pltpu.VMEM((blocks, ghosts), BF16),
            pltpu.VMEM((blocks, 2 * ghosts), BF16),
            pltpu.VMEM((half, *group), BF16),
            pltpu.VMEM((levels, *group), BF16),
            pltpu.VMEM((levels, *group), BF16),
            pltpu.VMEM((levels, *group), BF16),
            pltpu.VMEM((slots, comps * blocks, nodes), F32),
            pltpu.VMEM((comps * ghosts, faces_n * nodes), F32),
            pltpu.VMEM((comps, faces_n * ghosts, nodes), BF16),
            pltpu.VMEM((faces_n, *field), BF16),
            pltpu.VMEM((slots, comps * blocks, nodes), BF16),
            pltpu.VMEM((faces_n * ghosts, wide), F32),
            pltpu.VMEM((faces_n, comps * ghosts, nodes), BF16),
            pltpu.VMEM((comps, 2 * blocks, nodes), BF16),
            pltpu.VMEM(field, F32),
            pltpu.VMEM((1, nodes), F32),
            pltpu.VMEM((n_space, 1, nodes), F32),
            pltpu.VMEM((faces_n * ghosts, 4 * ghosts), BF16),
            pltpu.VMEM((faces_n * ghosts, 4 * ghosts), BF16),
            pltpu.VMEM((4, halo, nodes), BF16),
            pltpu.VMEM((4, halo, nodes), BF16),
            pltpu.VMEM((twos, *group), BF16),
            pltpu.VMEM((twos, 4, *group), BF16),
            pltpu.VMEM((comps, ghosts, nodes), BF16),
            dma((10,)),
            dma((half, 4)),
            dma((half, 4)),
            dma((levels, 4)),
            dma((levels, 4)),
            dma((3,)),
            dma((2, 2, half)),
            dma((n_dev,)),
            dma((n_space,)),
            dma((2, 4)),
            dma((2, 4)),
            dma((2, half // 2, 4)),
            dma((twos, 16)),
            dma((twos, 16)),
            pltpu.SemaphoreType.REGULAR((max(1, len(rounds_of(n_space))), 2)),
        ],
        compiler_params=pltpu.CompilerParams(
            collective_id=0, has_side_effects=True, vmem_limit_bytes=60 * 1024 * 1024
        ),
        name="window",
    )(pitch, mixing, checkpoints, sources, metric, obj_weight, adjoint_end, lift, faces.T, send_idx)
    return bounds, grad


def solution(mesh):
    placed = (
        P("tm", None, "space", None),
        P(None, None, "space", None),
        P(),
        P("space", None),
        P(None, "space", None),
        P(None, "space", None),
        P(),
        P(),
        P("space", None),
        P("space", None, None),
    )
    return jax.shard_map(
        shards,
        mesh=mesh,
        in_specs=placed,
        out_specs=(P("tm", None, "space", None), P()),
        check_vma=False,
    )
```

```python
import functools
import math

import jax
import jax.numpy as jnp
from jax import lax
from jax.experimental import pallas as pl
from jax.experimental.pallas import tpu as pltpu
from jax.sharding import PartitionSpec as P

OFFSETS = (1, -1, 2, -2)
STEP_SIZE = 0.5
F32 = jnp.float32
BF16 = jnp.bfloat16
MESH = pl.DeviceIdType.MESH
DIRS = range(4)


def dot(a, b):
    return jnp.dot(a, b, preferred_element_type=F32)


def one_hot(hit):
    return hit.astype(F32).astype(BF16)


def beside(parts):
    return jnp.concatenate(list(parts), axis=1)


def below(parts):
    return jnp.concatenate(list(parts), axis=0)


def rounds_of(n_space):
    reach, rounds = 2 * max(OFFSETS), []
    while reach < n_space - 1:
        rounds.append(reach)
        reach *= 2
    return rounds


def window_kernel(
    dims,
    pitch_hbm, mixing_hbm, cp_hbm, src_hbm, metric_hbm, weight_hbm, end_hbm, lift_hbm, faces_hbm, send_hbm,
    out_ref, grad_ref,
    pitch_ref, mixing_ref, u_ref, lift_ref, faces_ref, send_ref, src_ref, metric_ref, weight_ref, a_ref, hand_ref,
    base_ref, dd_ref, wu_ref, lift_t, sq_ref,
    p_own, p_halo, pt_own, pt_halo, pick, pick_t, pick_t2, out_buf, in_buf, back_out, back_in, y_ref, yh_ref, z_ref,
    mixed_ref, g_ref, gw_ref, gh_ref, split_ref, wf_ref, row_ref, rows_ref,
    et_out, et_in, mg_out, mg_in, dup_out, dup_in, last_ref, turn_ref, part_ref, hint_out, hint_in,
    load_sems, send_sems, recv_sems, bsend_sems, brecv_sems, hand_sems, factor_sems, gsend_sems, grecv_sems,
    table_sems, metric_sems, ghost_sems, dsend_sems, drecv_sems, round_sems, hint_sems, keep_sems,
):
    comps, blocks, nodes, slots, halo, half, n_tm, n_space, norm = dims
    ghosts = 4 * halo
    faces_n = slots - 1
    tm = lax.axis_index("tm")
    sp = lax.axis_index("space")
    n_dev = n_tm * n_space
    me = tm * n_space + sp
    lead = tm == n_tm - 1
    partner = (n_tm - 1 - tm, sp)
    levels = half * n_tm
    rounds = rounds_of(n_space)
    chunk = 32

    pairs = [
        (send_hbm, send_ref),
        (cp_hbm.at[0], u_ref),
        (faces_hbm, faces_ref),
        (pitch_hbm, pitch_ref),
        (mixing_hbm, mixing_ref),
        (lift_hbm, lift_ref),
        (metric_hbm, metric_ref),
        (weight_hbm, weight_ref),
        (src_hbm, src_ref),
        (end_hbm, a_ref),
    ]
    loads = [pltpu.make_async_copy(src, dst, load_sems.at[i]) for i, (src, dst) in enumerate(pairs)]
    for load in loads:
        load.start()

    in_buf[...] = jnp.zeros_like(in_buf)

    @pl.when(lead)
    def _():
        et_in[...] = jnp.zeros_like(et_in)
        mg_in[...] = jnp.zeros_like(mg_in)
        hint_in[...] = jnp.zeros_like(hint_in)

    barrier = pltpu.get_barrier_semaphore()

    def inside(shift):
        return (sp + shift >= 0) & (sp + shift < n_space)

    def at(shift):
        return jnp.clip(sp + shift, 0, n_space - 1)

    met = n_tm - 1
    pl.semaphore_signal(barrier, inc=1, device_id=partner, device_id_type=MESH)
    for shift in OFFSETS:
        met = met + n_tm * inside(shift).astype(jnp.int32)

        @pl.when(inside(shift))
        def _():
            for side in range(n_tm):
                pl.semaphore_signal(barrier, inc=1, device_id=(side, at(shift)), device_id_type=MESH)

    def lanes(c):
        return slice(c * nodes, (c + 1) * nodes)

    def target(shift):
        return (tm, at(shift))

    def forward_copy(n, d):
        return pltpu.make_async_remote_copy(
            src_ref=out_buf.at[n, d], dst_ref=in_buf.at[tm * half + n, d],
            send_sem=send_sems.at[n, d], recv_sem=recv_sems.at[n, d],
            device_id=target(OFFSETS[d]), device_id_type=MESH,
        )

    def ghost_copy(n, d):
        return pltpu.make_async_remote_copy(
            src_ref=out_buf.at[n, d], dst_ref=in_buf.at[n, d],
            send_sem=ghost_sems.at[0, n // 2, d], recv_sem=ghost_sems.at[1, n // 2, d],
            device_id=(n_tm - 1, at(OFFSETS[d])), device_id_type=MESH,
        )

    def hint_copy(d):
        return pltpu.make_async_remote_copy(
            src_ref=hint_out.at[d], dst_ref=hint_in.at[d],
            send_sem=hint_sems.at[0, d], recv_sem=hint_sems.at[1, d],
            device_id=(n_tm - 1, at(OFFSETS[d])), device_id_type=MESH,
        )

    def metric_copy(d):
        return pltpu.make_async_remote_copy(
            src_ref=mg_out.at[d], dst_ref=mg_in.at[d],
            send_sem=metric_sems.at[0, d], recv_sem=metric_sems.at[1, d],
            device_id=target(OFFSETS[d]), device_id_type=MESH,
        )

    def table_copy(d):
        rows = pl.ds(d * faces_n * halo, faces_n * halo)
        return pltpu.make_async_remote_copy(
            src_ref=et_out.at[rows], dst_ref=et_in.at[rows],
            send_sem=table_sems.at[0, d], recv_sem=table_sems.at[1, d],
            device_id=target(-OFFSETS[d]), device_id_type=MESH,
        )

    def second_copy(slot, d, far):
        return pltpu.make_async_remote_copy(
            src_ref=dup_out.at[slot, far], dst_ref=dup_in.at[slot, d, far],
            send_sem=dsend_sems.at[slot, 4 * d + far], recv_sem=drecv_sems.at[slot, 4 * d + far],
            device_id=target(-OFFSETS[far] - OFFSETS[d]), device_id_type=MESH,
        )

    second_pairs = [(d, far) for d in DIRS for far in DIRS if OFFSETS[d] + OFFSETS[far] != 0]
    second_pairs = sorted(second_pairs, key=lambda p: -abs(OFFSETS[p[0]] + OFFSETS[p[1]]))

    def backward_copy(n, d):
        return pltpu.make_async_remote_copy(
            src_ref=back_out.at[n, d], dst_ref=back_in.at[n, d],
            send_sem=bsend_sems.at[n, d], recv_sem=brecv_sems.at[n, d],
            device_id=target(-OFFSETS[d]), device_id_type=MESH,
        )

    def coef(k, e, c):
        return mixing_ref[k, e, c]

    def turn_of(level):
        angle = jnp.full((8, nodes), pitch_ref[level], F32)
        return jnp.cos(angle)[0:1], jnp.sin(angle)[0:1]

    def ghost_rows(ref, index, c):
        return below(ref[index + (d, c)] for d in DIRS)

    def ghost_wide(ref, index):
        return beside(ghost_rows(ref, index, c) for c in range(comps))

    def squash_and_pick(n):
        for c in range(comps):
            sq_ref[c] = jnp.tanh(u_ref[c]).astype(BF16)
        picked = dot(pick[...], beside(sq_ref[c] for c in range(comps))).astype(BF16)
        for d in DIRS:
            for c in range(comps):
                out_buf[n, d, c] = picked[d * halo : (d + 1) * halo, lanes(c)]

    row_ids = lax.broadcasted_iota(jnp.int32, (blocks, blocks), 0)
    lane_ids = lax.broadcasted_iota(jnp.int32, (blocks, blocks), 1)
    loads[0].wait()
    wanted = beside(
        [send_ref[0, d : d + 1, :] for d in DIRS] + [jnp.full((1, blocks - ghosts), -1, jnp.int32)]
    )
    spread = jnp.broadcast_to(wanted, (blocks, blocks))
    spread_t = jnp.transpose(spread.astype(F32)).astype(jnp.int32)
    pick[...] = one_hot(spread_t[:ghosts] == lane_ids[:ghosts])
    loads[1].wait()
    squash_and_pick(0)
    pl.semaphore_wait(barrier, met)
    for d in DIRS:
        @pl.when(inside(OFFSETS[d]))
        def _():
            forward_copy(0, d).start()

    pick_t[...] = one_hot(spread == row_ids)[:, :ghosts]
    doubled = beside([wanted[:, :ghosts]] * 2)
    pick_t2[...] = one_hot(jnp.broadcast_to(doubled, (blocks, 2 * ghosts)) == row_ids)
    part_ref[...] = jnp.zeros_like(part_ref)
    loads[2].wait()
    face_cols = []
    for k in range(faces_n):
        turned = jnp.broadcast_to(faces_ref[k : k + 1, :], (blocks, blocks))
        col = jnp.transpose(turned.astype(F32)).astype(jnp.int32)
        face_cols.append(col)
        p_own[k * blocks : (k + 1) * blocks, :] = one_hot(col == lane_ids)
        pt_own[k * blocks : (k + 1) * blocks, :] = one_hot(turned == row_ids)
        hit = one_hot(turned[:ghosts] == row_ids[:ghosts] + blocks)
        pt_halo[k * ghosts : (k + 1) * ghosts, :blocks] = hit
        pt_halo[k * ghosts : (k + 1) * ghosts, blocks:] = hit
    for pair in range(faces_n // 2):
        low = lane_ids < ghosts
        col = jnp.where(low, face_cols[2 * pair], face_cols[2 * pair + 1])
        want = jnp.where(low, lane_ids, lane_ids - ghosts) + blocks
        p_halo[:, pair * 2 * ghosts : (pair + 1) * 2 * ghosts] = one_hot(col == want)

    for load in loads[3:]:
        load.wait()
    for k in range(slots):
        lift_t[:, k * nodes : (k + 1) * nodes] = jnp.transpose(lift_ref[k].astype(F32)).astype(BF16)

    @pl.when(lead)
    def _():
        which = lax.broadcasted_iota(jnp.int32, (levels, nodes), 0)
        angles = jnp.zeros((levels, nodes), F32)
        for n in range(levels):
            angles = jnp.where(which == n, pitch_ref[n], angles)
        turn_ref[0] = jnp.cos(angles)
        turn_ref[1] = jnp.sin(angles)
        back_in[...] = jnp.zeros_like(back_in)
        dup_in[...] = jnp.zeros_like(dup_in)
        four = beside([wanted[:, :ghosts]] * 4)
        ids = lax.broadcasted_iota(jnp.int32, (blocks, 4 * ghosts), 0)
        picks = one_hot(jnp.broadcast_to(four, (blocks, 4 * ghosts)) == ids)
        table = dot(pt_halo[:, :blocks], picks)
        part = lax.broadcasted_iota(jnp.int32, (halo, 4 * ghosts), 1) // ghosts
        for d in DIRS:
            for k in range(faces_n):
                piece = table[k * ghosts + d * halo : k * ghosts + (d + 1) * halo]
                to = (d * faces_n + k) * halo
                et_out[to : to + halo, :] = jnp.where(part == d, piece, 0.0).astype(BF16)
        chosen = dot(pick[...], metric_ref[...].astype(BF16)).astype(BF16)
        for d in DIRS:
            mg_out[d] = chosen[d * halo : (d + 1) * halo]
        for d in DIRS:
            @pl.when(inside(OFFSETS[d]))
            def _():
                metric_copy(d).start()

            @pl.when(inside(-OFFSETS[d]))
            def _():
                table_copy(d).start()

    def factor_copy(level, which):
        ref = (dd_ref, wu_ref)[which]
        return pltpu.make_async_remote_copy(
            src_ref=ref.at[level], dst_ref=ref.at[level], send_sem=factor_sems.at[0, which, level],
            recv_sem=factor_sems.at[1, which, level], device_id=partner, device_id_type=MESH,
        )

    def round_signal(r):
        for side, shift in enumerate((rounds[r], -rounds[r])):
            @pl.when(inside(shift))
            def _():
                pl.semaphore_signal(
                    round_sems.at[r, side], inc=1, device_id=(n_tm - 1, at(shift)), device_id_type=MESH
                )

    def round_wait(r):
        for side, shift in enumerate((rounds[r], -rounds[r])):
            @pl.when(inside(-shift))
            def _():
                pl.semaphore_wait(round_sems.at[r, side], 1)

    def round_step(r):
        if 0 < r <= len(rounds):
            round_wait(r - 1)
        if r < len(rounds):
            round_signal(r)

    def forward(n, carry):
        level = tm * half + n
        active = (n < half - 1) | lead

        @pl.when(n > 0)
        def _():
            squash_and_pick(n)
            for d in DIRS:
                @pl.when(inside(OFFSETS[d]) & active)
                def _():
                    forward_copy(n, d).start()

                @pl.when(inside(OFFSETS[d]) & jnp.logical_not(lead) & (lax.rem(n, 2) == 1))
                def _():
                    ghost_copy(n, d).start()

        for r in range(half - 1):
            @pl.when(lead & (n == r + 1))
            def _():
                round_step(r)

        keep = jnp.where(level > 0, 1.0, 0.0).astype(F32)
        for c in range(comps):
            state = u_ref[c]
            t = jnp.tanh(state)
            dd_ref[level, c] = STEP_SIZE * (1.0 - t * t)
            wu_ref[level, c] = (keep * weight_ref[c]) * state

        @pl.when(jnp.logical_not(lead))
        def _():
            factor_copy(level, 0).start()
            factor_copy(level, 1).start()

        @pl.when(level == 1)
        def _():
            cosine, sine = turn_of(0)
            fields = []
            for c in range(comps):
                turning = cosine * src_ref[1, c] - sine * src_ref[0, c]
                fields.append((dd_ref[1, c] * turning).astype(BF16))
            chosen = dot(pick[...], beside(fields)).astype(BF16)
            for d in DIRS:
                for c in range(comps):
                    hint_out[d, c] = chosen[d * halo : (d + 1) * halo, lanes(c)]
            for d in DIRS:
                @pl.when(inside(OFFSETS[d]))
                def _():
                    hint_copy(d).start()

        @pl.when(active)
        def _():
            cosine, sine = turn_of(level)
            squashed = beside(sq_ref[c] for c in range(comps))
            for k in range(slots):
                if k == 0:
                    stacked = sq_ref[...].reshape(comps * blocks, nodes)
                else:
                    got = dot(p_own[(k - 1) * blocks : k * blocks, :], squashed).astype(BF16)
                    stacked = below(got[:, lanes(c)] for c in range(comps))
                y_ref[k] = dot(stacked, lift_t[:, lanes(k)])

            def own_mix(r, carry):
                start = pl.multiple_of(r * chunk, chunk)
                metric_half = STEP_SIZE * metric_ref[pl.ds(start, chunk), :]
                sums = [None] * comps
                for k in range(slots):
                    for c in range(comps):
                        term = y_ref[k, pl.ds(c * blocks + start, chunk), :]
                        for e in range(comps):
                            add = coef(k, e, c) * term
                            sums[e] = add if sums[e] is None else sums[e] + add
                for e in range(comps):
                    rows = pl.ds(start, chunk)
                    forcing = cosine * src_ref[0, e, rows, :] + sine * src_ref[1, e, rows, :]
                    base_ref[e, rows, :] = u_ref[e, rows, :] + STEP_SIZE * forcing - metric_half * sums[e]
                return carry

            lax.fori_loop(0, blocks // chunk, own_mix, 0)

            for d in DIRS:
                @pl.when(inside(OFFSETS[d]))
                def _():
                    forward_copy(n, d).wait_send()

            for d in DIRS:
                @pl.when(inside(-OFFSETS[d]))
                def _():
                    forward_copy(n, d).wait_recv()

            stacked = below(ghost_rows(in_buf, (level,), c) for c in range(comps))
            yh_ref[...] = dot(stacked, lift_t[:, nodes:])
            for k in range(1, slots):
                for part in range(ghosts // chunk):
                    for e in range(comps):
                        total = None
                        for c in range(comps):
                            row = c * ghosts + part * chunk
                            add = coef(k, e, c) * yh_ref[row : row + chunk, lanes(k - 1)]
                            total = add if total is None else total + add
                        row = (k - 1) * ghosts + part * chunk
                        z_ref[e, row : row + chunk, :] = total.astype(BF16)
            more = dot(p_halo[...], beside(z_ref[e] for e in range(comps)))
            half_metric = STEP_SIZE * metric_ref[...]
            for e in range(comps):
                u_ref[e] = base_ref[e] - half_metric * more[:, lanes(e)]

        return carry

    lax.fori_loop(0, half, forward, 0)

    def hand_copy(c):
        return pltpu.make_async_remote_copy(
            src_ref=a_ref.at[c], dst_ref=out_ref.at[0, c], send_sem=hand_sems.at[0, c], recv_sem=hand_sems.at[1, c],
            device_id=partner, device_id_type=MESH,
        )

    def keep_copy():
        return pltpu.make_async_copy(hand_ref, out_ref.at[0], keep_sems)

    def grad_copy(source, other):
        return pltpu.make_async_remote_copy(
            src_ref=row_ref, dst_ref=rows_ref.at[source], send_sem=gsend_sems.at[other],
            recv_sem=grecv_sems.at[source], device_id=(other // n_space, lax.rem(other, n_space)),
            device_id_type=MESH,
        )

    def mix_back(k, row, rows, to):
        for c in range(comps):
            total = None
            for e in range(comps):
                add = coef(k, e, c) * gw_ref[row : row + rows, lanes(e)]
                total = add if total is None else total + add
            gh_ref[k - 1, c * ghosts + to : c * ghosts + to + rows, :] = total.astype(BF16)

    def lift_back():
        return dot(beside(gh_ref[k] for k in range(faces_n)), lift_ref[1:].reshape(faces_n * nodes, nodes))

    def halo_part(ref, level, keep):
        for e in range(comps):
            w = metric_ref[...] * ref[e]
            if keep:
                wf_ref[e] = w
            high = w.astype(BF16)
            split_ref[e, :blocks, :] = high
            split_ref[e, blocks:, :] = (w - high.astype(F32)).astype(BF16)
        gw_ref[...] = dot(pt_halo[...], beside(split_ref[e] for e in range(comps)))
        for k in range(1, slots):
            for part in range(ghosts // chunk):
                mix_back(k, (k - 1) * ghosts + part * chunk, chunk, part * chunk)
        lifted = lift_back().astype(BF16)
        for d in DIRS:
            for c in range(comps):
                row = c * ghosts + d * halo
                back_out[level, d, c] = lifted[row : row + halo]
        for d in DIRS:
            @pl.when(inside(-OFFSETS[d]))
            def _():
                backward_copy(level, d).start()

    def own_mixing():
        for k in [*range(1, slots), 0]:
            for r in range(blocks // chunk):
                rows = slice(r * chunk, (r + 1) * chunk)
                weighted = [wf_ref[e, rows, :] for e in range(comps)]
                for c in range(comps):
                    total = None
                    for e in range(comps):
                        add = coef(k, e, c) * weighted[e]
                        total = add if total is None else total + add
                    if k == 0:
                        g_ref[0, c * blocks + r * chunk : c * blocks + (r + 1) * chunk, :] = total.astype(BF16)
                    else:
                        mixed_ref[k - 1, c, rows, :] = total.astype(BF16)
            if k > 0:
                wide = beside(mixed_ref[k - 1, c] for c in range(comps))
                got = dot(pt_own[(k - 1) * blocks : k * blocks, :], wide).astype(BF16)
                for c in range(comps):
                    g_ref[k, c * blocks : (c + 1) * blocks, :] = got[:, lanes(c)]

    def own_lift(level):
        pushed = dot(beside(g_ref[k] for k in range(slots)), lift_ref[...].reshape(slots * nodes, nodes))
        for c in range(comps):
            base_ref[c] = a_ref[c] + wu_ref[level, c] - dd_ref[level, c] * pushed[c * blocks : (c + 1) * blocks]

    def add_grad(level, ref=a_ref, extra=None):
        cosine, sine = turn_ref[0, pl.ds(level, 1), :], turn_ref[1, pl.ds(level, 1), :]
        sums = extra
        for e in range(comps):
            part = ref[e] * (cosine * src_ref[1, e] - sine * src_ref[0, e])
            sums = part if sums is None else sums + part
        part_ref[pl.ds(level, 1), :] = jnp.sum(sums, axis=0, keepdims=True)

    def total_grad():
        values = jnp.sum(part_ref[...], axis=1, keepdims=True) * (STEP_SIZE / norm)
        spots = lax.broadcasted_iota(jnp.int32, (levels, nodes), 1)
        own = lax.broadcasted_iota(jnp.int32, (levels, nodes), 0)
        row_ref[...] = jnp.sum(jnp.where(spots == own, values, 0.0), axis=0, keepdims=True)

    def backward(j, carry):
        high = levels - 1 - 2 * j
        low = high - 1

        halo_part(a_ref, high, True)

        @pl.when(j == 0)
        def _():
            for d in DIRS:
                @pl.when(inside(-OFFSETS[d]))
                def _():
                    metric_copy(d).wait_recv()

        @pl.when(high < half)
        def _():
            for d in DIRS:
                @pl.when(inside(-OFFSETS[d]))
                def _():
                    ghost_copy(high, d).wait_recv()

            for which in range(2):
                factor_copy(high, which).wait_recv()
                factor_copy(low, which).wait_recv()

        for far in DIRS:
            spread_metric = mg_in[far].astype(F32)
            d = OFFSETS.index(-OFFSETS[far])
            for c in range(comps):
                t = in_buf[high, far, c].astype(F32)
                factor = spread_metric * (STEP_SIZE - STEP_SIZE * t * t)
                scaled = (factor * back_out[high, far, c].astype(F32)).astype(BF16)
                dup_out[j, far, c] = scaled
                dup_in[j, d, far, c] = scaled
        for d, far in second_pairs:
            @pl.when(inside(-OFFSETS[far]) & inside(-OFFSETS[far] - OFFSETS[d]))
            def _():
                second_copy(j, d, far).start()

        add_grad(high)
        own_mixing()
        own_lift(high)
        halo_part(base_ref, low, False)

        @pl.when(low == 0)
        def _():
            for d in DIRS:
                @pl.when(inside(-OFFSETS[d]))
                def _():
                    hint_copy(d).wait_recv()

            missing = None
            for d in DIRS:
                for c in range(comps):
                    part = back_out[high, d, c].astype(F32) * hint_in[d, c].astype(F32)
                    missing = part if missing is None else missing + part
            add_grad(low, base_ref, below([-missing, jnp.zeros((blocks - halo, nodes), F32)]))
            total_grad()

            def tell(r, carry):
                other = lax.rem(me + r, n_dev)
                grad_copy(sp, other).start()
                return carry

            lax.fori_loop(1, n_dev, tell, 0)

        for d in DIRS:
            @pl.when(inside(OFFSETS[d]))
            def _():
                backward_copy(high, d).wait_recv()

        more = dot(pick_t[...], ghost_wide(back_in, (high,)))
        for c in range(comps):
            state = base_ref[c] - dd_ref[high, c] * more[:, lanes(c)]
            a_ref[c] = state
            wf_ref[c] = metric_ref[...] * state

        add_grad(low)

        own_mixing()
        own_lift(low)

        @pl.when(j == 0)
        def _():
            for d in DIRS:
                @pl.when(inside(OFFSETS[d]))
                def _():
                    table_copy(d).wait_recv()

        for d, far in second_pairs:
            @pl.when(inside(OFFSETS[d]) & inside(OFFSETS[d] + OFFSETS[far]))
            def _():
                second_copy(j, d, far).wait_recv()

        rows = [below(dup_in[j, d, far, c] for d in DIRS for far in DIRS) for c in range(comps)]
        gw_ref[...] = dot(et_in[...], beside(rows))
        for k in range(1, slots):
            for d in DIRS:
                mix_back(k, (d * faces_n + k - 1) * halo, halo, d * halo)
        lifted = (-lift_back()).astype(BF16)
        for c in range(comps):
            last_ref[c] = lifted[c * ghosts : (c + 1) * ghosts]

        for d in DIRS:
            @pl.when(inside(OFFSETS[d]))
            def _():
                backward_copy(low, d).wait_recv()

        late = beside(below([ghost_rows(back_in, (low,), c), last_ref[c]]) for c in range(comps))
        more = dot(pick_t2[...], late)
        for c in range(comps):
            a_ref[c] = base_ref[c] - dd_ref[low, c] * more[:, lanes(c)]

        @pl.when(low == half)
        def _():
            for c in range(comps):
                hand_ref[c] = a_ref[c]
            keep_copy().start()

        return carry

    @pl.when(lead)
    def _():
        for r in range(half - 1, len(rounds) + 1):
            round_step(r)
        for c in range(comps):
            a_ref[c] = a_ref[c] + weight_ref[c] * u_ref[c]
        lax.fori_loop(0, levels // 2, backward, 0)
        for c in range(comps):
            hand_copy(c).start()
        rows_ref[sp] = row_ref[...]

        def drained(j, carry):
            for d, far in second_pairs:
                @pl.when(inside(-OFFSETS[far]) & inside(-OFFSETS[far] - OFFSETS[d]))
                def _():
                    second_copy(j, d, far).wait_send()
            for d in DIRS:
                @pl.when(inside(-OFFSETS[d]))
                def _():
                    backward_copy(2 * j, d).wait_send()
                    backward_copy(2 * j + 1, d).wait_send()
            return carry

        lax.fori_loop(0, levels // 2, drained, 0)
        for d in DIRS:
            @pl.when(inside(OFFSETS[d]))
            def _():
                metric_copy(d).wait_send()

            @pl.when(inside(-OFFSETS[d]))
            def _():
                table_copy(d).wait_send()

        def settle(r, carry):
            other = lax.rem(sp + r, n_space)
            grad_copy(other, me).wait_recv()
            return carry

        lax.fori_loop(1, n_space, settle, 0)

    @pl.when(jnp.logical_not(lead))
    def _():
        def settle(r, carry):
            grad_copy(r, me).wait_recv()
            return carry

        lax.fori_loop(0, n_space, settle, 0)

    grad_ref[...] = jnp.sum(rows_ref[...], axis=0)[0, : grad_ref.shape[0]]

    @pl.when(lead)
    def _():
        for c in range(comps):
            hand_copy(c).wait_send()
        keep_copy().wait()

        def sent(r, carry):
            grad_copy(sp, lax.rem(me + r, n_dev)).wait_send()
            return carry

        lax.fori_loop(1, n_dev, sent, 0)

    @pl.when(jnp.logical_not(lead))
    def _():
        for c in range(comps):
            hand_copy(c).wait_recv()
        for level in range(half):
            factor_copy(level, 0).wait_send()
            factor_copy(level, 1).wait_send()
        for d in DIRS:
            @pl.when(inside(OFFSETS[d]))
            def _():
                hint_copy(d).wait_send()
                for level in range(1, half, 2):
                    ghost_copy(level, d).wait_send()


def finish_kernel(pieces, held_hbm, grad_hbm, out_hbm, grad_out, buf, row, sems):
    inward = [pltpu.make_async_copy(held_hbm.at[0, c], buf.at[c], sems.at[0, c]) for c in range(pieces)]
    outward = [pltpu.make_async_copy(buf.at[c], out_hbm.at[0, c], sems.at[1, c]) for c in range(pieces)]
    inward.append(pltpu.make_async_copy(grad_hbm, row, sems.at[0, pieces]))
    outward.append(pltpu.make_async_copy(row, grad_out, sems.at[1, pieces]))
    for copy in inward:
        copy.start()
    for first, second in zip(inward, outward):
        first.wait()
        second.start()
    for copy in outward:
        copy.wait()


def shards(
    checkpoints, sources, pitch, metric, obj_weight, adjoint_end, lift, mixing, faces, send_idx
):
    comps = sources.shape[1]
    blocks, nodes = metric.shape
    slots = lift.shape[0]
    faces_n = slots - 1
    halo = send_idx.shape[2]
    n_tm = lax.axis_size("tm")
    n_space = lax.axis_size("space")
    levels = pitch.shape[0]
    half = levels // n_tm
    twos = levels // 2
    ghosts = 4 * halo
    norm = math.sqrt(comps * nodes * blocks * n_space)
    wide = comps * nodes
    field = (comps, blocks, nodes)
    group = (4, comps, halo, nodes)
    vmem = pl.BlockSpec(memory_space=pltpu.VMEM)
    anym = pl.BlockSpec(memory_space=pl.ANY)
    dma = pltpu.SemaphoreType.DMA
    n_dev = n_tm * n_space
    dims = (comps, blocks, nodes, slots, halo, half, n_tm, n_space, norm)
    bounds, grad = pl.pallas_call(
        functools.partial(window_kernel, dims),
        out_shape=(
            jax.ShapeDtypeStruct((1, *field), F32),
            jax.ShapeDtypeStruct((levels,), F32),
        ),
        in_specs=[anym] * 10,
        out_specs=(anym, vmem),
        scratch_shapes=[
            pltpu.SMEM(pitch.shape, F32),
            pltpu.SMEM(mixing.shape, F32),
            pltpu.VMEM(field, F32),
            pltpu.VMEM(lift.shape, BF16),
            pltpu.VMEM(faces.shape[::-1], jnp.int32),
            pltpu.VMEM(send_idx.shape, jnp.int32),
            pltpu.VMEM((2, *field), F32),
            pltpu.VMEM((blocks, nodes), F32),
            pltpu.VMEM(field, F32),
            pltpu.VMEM(field, F32),
            pltpu.VMEM(field, F32),
            pltpu.VMEM(field, F32),
            pltpu.VMEM((levels, *field), F32),
            pltpu.VMEM((levels, *field), F32),
            pltpu.VMEM((nodes, slots * nodes), BF16),
            pltpu.VMEM(field, BF16),
            pltpu.VMEM((faces_n * blocks, blocks), BF16),
            pltpu.VMEM((blocks, faces_n * ghosts), BF16),
            pltpu.VMEM((faces_n * blocks, blocks), BF16),
            pltpu.VMEM((faces_n * ghosts, 2 * blocks), BF16),
            pltpu.VMEM((ghosts, blocks), BF16),
            pltpu.VMEM((blocks, ghosts), BF16),
            pltpu.VMEM((blocks, 2 * ghosts), BF16),
            pltpu.VMEM((half, *group), BF16),
            pltpu.VMEM((levels, *group), BF16),
            pltpu.VMEM((levels, *group), BF16),
            pltpu.VMEM((levels, *group), BF16),
            pltpu.VMEM((slots, comps * blocks, nodes), F32),
            pltpu.VMEM((comps * ghosts, faces_n * nodes), F32),
            pltpu.VMEM((comps, faces_n * ghosts, nodes), BF16),
            pltpu.VMEM((faces_n, *field), BF16),
            pltpu.VMEM((slots, comps * blocks, nodes), BF16),
            pltpu.VMEM((faces_n * ghosts, wide), F32),
            pltpu.VMEM((faces_n, comps * ghosts, nodes), BF16),
            pltpu.VMEM((comps, 2 * blocks, nodes), BF16),
            pltpu.VMEM(field, F32),
            pltpu.VMEM((1, nodes), F32),
            pltpu.VMEM((n_space, 1, nodes), F32),
            pltpu.VMEM((faces_n * ghosts, 4 * ghosts), BF16),
            pltpu.VMEM((faces_n * ghosts, 4 * ghosts), BF16),
            pltpu.VMEM((4, halo, nodes), BF16),
            pltpu.VMEM((4, halo, nodes), BF16),
            pltpu.VMEM((twos, *group), BF16),
            pltpu.VMEM((twos, 4, *group), BF16),
            pltpu.VMEM((comps, ghosts, nodes), BF16),
            pltpu.VMEM((2, levels, nodes), F32),
            pltpu.VMEM((levels, nodes), F32),
            pltpu.VMEM(group, BF16),
            pltpu.VMEM(group, BF16),
            dma((10,)),
            dma((half, 4)),
            dma((half, 4)),
            dma((levels, 4)),
            dma((levels, 4)),
            dma((2, comps)),
            dma((2, 2, half)),
            dma((n_dev,)),
            dma((n_space,)),
            dma((2, 4)),
            dma((2, 4)),
            dma((2, half // 2, 4)),
            dma((twos, 16)),
            dma((twos, 16)),
            pltpu.SemaphoreType.REGULAR((max(1, len(rounds_of(n_space))), 2)),
            dma((2, 4)),
            dma(()),
        ],
        compiler_params=pltpu.CompilerParams(
            collective_id=0, has_side_effects=True, vmem_limit_bytes=60 * 1024 * 1024
        ),
        name="window",
    )(pitch, mixing, checkpoints, sources, metric, obj_weight, adjoint_end, lift, faces.T, send_idx)
    return pl.pallas_call(
        functools.partial(finish_kernel, comps),
        out_shape=(
            jax.ShapeDtypeStruct((1, *field), F32),
            jax.ShapeDtypeStruct((levels,), F32),
        ),
        in_specs=[anym] * 2,
        out_specs=(anym, anym),
        scratch_shapes=[pltpu.VMEM(field, F32), pltpu.VMEM((levels,), F32), dma((2, comps + 1))],
        compiler_params=pltpu.CompilerParams(vmem_limit_bytes=60 * 1024 * 1024),
        name="finish",
    )(bounds, grad)


def solution(mesh):
    placed = (
        P("tm", None, "space", None),
        P(None, None, "space", None),
        P(),
        P("space", None),
        P(None, "space", None),
        P(None, "space", None),
        P(),
        P(),
        P("space", None),
        P("space", None, None),
    )
    return jax.shard_map(
        shards,
        mesh=mesh,
        in_specs=placed,
        out_specs=(P("tm", None, "space", None), P()),
        check_vma=False,
    )
```

```python
import functools
import math

import jax
import jax.numpy as jnp
from jax import lax
from jax.experimental import pallas as pl
from jax.experimental.pallas import tpu as pltpu
from jax.sharding import PartitionSpec as P

OFFSETS = (1, -1, 2, -2)
STEP_SIZE = 0.5
F32 = jnp.float32
BF16 = jnp.bfloat16
MESH = pl.DeviceIdType.MESH
DIRS = range(4)


def dot(a, b):
    return jnp.dot(a, b, preferred_element_type=F32)


def one_hot(hit):
    return hit.astype(F32).astype(BF16)


def beside(parts):
    return jnp.concatenate(list(parts), axis=1)


def below(parts):
    return jnp.concatenate(list(parts), axis=0)


def rounds_of(n_space):
    reach, rounds = 2 * max(OFFSETS), []
    while reach < n_space - 1:
        rounds.append(reach)
        reach *= 2
    return rounds


def window_kernel(
    dims,
    pitch_hbm, mixing_hbm, cp_hbm, src_hbm, metric_hbm, weight_hbm, end_hbm, lift_hbm, faces_hbm, send_hbm,
    out_ref, grad_ref,
    pitch_ref, mixing_ref, u_ref, lift_ref, faces_ref, send_ref, src_ref, metric_ref, weight_ref, a_ref, hand_ref,
    base_ref, dd_ref, wu_ref, lift_t, sq_ref,
    p_own, p_halo, pt_own, pt_halo, pick, pick_t, pick_t2, out_buf, in_buf, back_out, back_in, y_ref, yh_ref, z_ref,
    mixed_ref, g_ref, gw_ref, gh_ref, split_ref, wf_ref, row_ref, rows_ref,
    et_out, et_in, mg_out, mg_in, dup_out, dup_in, last_ref, turn_ref, part_ref, hint_out, hint_in, near_ref, spot_metric, spot_base,
    load_sems, send_sems, recv_sems, bsend_sems, brecv_sems, hand_sems, factor_sems, gsend_sems, grecv_sems,
    table_sems, metric_sems, ghost_sems, dsend_sems, drecv_sems, round_sems, hint_sems, keep_sems,
):
    comps, blocks, nodes, slots, halo, half, n_tm, n_space, norm = dims
    ghosts = 4 * halo
    faces_n = slots - 1
    tm = lax.axis_index("tm")
    sp = lax.axis_index("space")
    n_dev = n_tm * n_space
    me = tm * n_space + sp
    lead = tm == n_tm - 1
    partner = (n_tm - 1 - tm, sp)
    levels = half * n_tm
    rounds = rounds_of(n_space)
    chunk = 32

    pairs = [
        (send_hbm, send_ref),
        (cp_hbm.at[0], u_ref),
        (faces_hbm, faces_ref),
        (pitch_hbm, pitch_ref),
        (mixing_hbm, mixing_ref),
        (lift_hbm, lift_ref),
        (metric_hbm, metric_ref),
        (weight_hbm, weight_ref),
        (src_hbm, src_ref),
        (end_hbm, a_ref),
    ]
    loads = [pltpu.make_async_copy(src, dst, load_sems.at[i]) for i, (src, dst) in enumerate(pairs)]
    for load in loads:
        load.start()

    in_buf[...] = jnp.zeros_like(in_buf)

    @pl.when(lead)
    def _():
        et_in[...] = jnp.zeros_like(et_in)
        mg_in[...] = jnp.zeros_like(mg_in)
        hint_in[...] = jnp.zeros_like(hint_in)

    barrier = pltpu.get_barrier_semaphore()

    def inside(shift):
        return (sp + shift >= 0) & (sp + shift < n_space)

    def at(shift):
        return jnp.clip(sp + shift, 0, n_space - 1)

    met = n_tm - 1
    pl.semaphore_signal(barrier, inc=1, device_id=partner, device_id_type=MESH)
    for shift in OFFSETS:
        met = met + n_tm * inside(shift).astype(jnp.int32)

        @pl.when(inside(shift))
        def _():
            for side in range(n_tm):
                pl.semaphore_signal(barrier, inc=1, device_id=(side, at(shift)), device_id_type=MESH)

    def lanes(c):
        return slice(c * nodes, (c + 1) * nodes)

    def target(shift):
        return (tm, at(shift))

    def forward_copy(n, d):
        return pltpu.make_async_remote_copy(
            src_ref=out_buf.at[n, d], dst_ref=in_buf.at[tm * half + n, d],
            send_sem=send_sems.at[n, d], recv_sem=recv_sems.at[n, d],
            device_id=target(OFFSETS[d]), device_id_type=MESH,
        )

    def ghost_copy(n, d):
        return pltpu.make_async_remote_copy(
            src_ref=out_buf.at[n, d], dst_ref=in_buf.at[n, d],
            send_sem=ghost_sems.at[0, n // 2, d], recv_sem=ghost_sems.at[1, n // 2, d],
            device_id=(n_tm - 1, at(OFFSETS[d])), device_id_type=MESH,
        )

    def hint_copy(d):
        return pltpu.make_async_remote_copy(
            src_ref=hint_out.at[d], dst_ref=hint_in.at[d],
            send_sem=hint_sems.at[0, d], recv_sem=hint_sems.at[1, d],
            device_id=(n_tm - 1, at(OFFSETS[d])), device_id_type=MESH,
        )

    def metric_copy(d):
        return pltpu.make_async_remote_copy(
            src_ref=mg_out.at[d], dst_ref=mg_in.at[d],
            send_sem=metric_sems.at[0, d], recv_sem=metric_sems.at[1, d],
            device_id=target(OFFSETS[d]), device_id_type=MESH,
        )

    def table_copy(d):
        rows = pl.ds(d * faces_n * halo, faces_n * halo)
        return pltpu.make_async_remote_copy(
            src_ref=et_out.at[rows], dst_ref=et_in.at[rows],
            send_sem=table_sems.at[0, d], recv_sem=table_sems.at[1, d],
            device_id=target(-OFFSETS[d]), device_id_type=MESH,
        )

    def second_copy(slot, d, far):
        return pltpu.make_async_remote_copy(
            src_ref=dup_out.at[slot, far], dst_ref=dup_in.at[slot, d, far],
            send_sem=dsend_sems.at[slot, 4 * d + far], recv_sem=drecv_sems.at[slot, 4 * d + far],
            device_id=target(-OFFSETS[far] - OFFSETS[d]), device_id_type=MESH,
        )

    second_pairs = [(d, far) for d in DIRS for far in DIRS if OFFSETS[d] + OFFSETS[far] != 0]
    second_pairs = sorted(second_pairs, key=lambda p: -abs(OFFSETS[p[0]] + OFFSETS[p[1]]))

    def backward_copy(n, d):
        return pltpu.make_async_remote_copy(
            src_ref=back_out.at[n, d], dst_ref=back_in.at[n, d],
            send_sem=bsend_sems.at[n, d], recv_sem=brecv_sems.at[n, d],
            device_id=target(-OFFSETS[d]), device_id_type=MESH,
        )

    def coef(k, e, c):
        return mixing_ref[k, e, c]

    def turn_of(level):
        angle = jnp.full((8, nodes), pitch_ref[level], F32)
        return jnp.cos(angle)[0:1], jnp.sin(angle)[0:1]

    def ghost_rows(ref, index, c):
        return below(ref[index + (d, c)] for d in DIRS)

    def ghost_wide(ref, index):
        return beside(ghost_rows(ref, index, c) for c in range(comps))

    def squash_and_pick(n):
        for c in range(comps):
            sq_ref[c] = jnp.tanh(u_ref[c]).astype(BF16)
        picked = dot(pick[...], beside(sq_ref[c] for c in range(comps))).astype(BF16)
        for d in DIRS:
            for c in range(comps):
                out_buf[n, d, c] = picked[d * halo : (d + 1) * halo, lanes(c)]

    row_ids = lax.broadcasted_iota(jnp.int32, (blocks, blocks), 0)
    lane_ids = lax.broadcasted_iota(jnp.int32, (blocks, blocks), 1)
    loads[0].wait()
    wanted = beside(
        [send_ref[0, d : d + 1, :] for d in DIRS] + [jnp.full((1, blocks - ghosts), -1, jnp.int32)]
    )
    spread = jnp.broadcast_to(wanted, (blocks, blocks))
    spread_t = jnp.transpose(spread.astype(F32)).astype(jnp.int32)
    pick[...] = one_hot(spread_t[:ghosts] == lane_ids[:ghosts])
    loads[1].wait()
    squash_and_pick(0)
    pl.semaphore_wait(barrier, met)
    for d in DIRS:
        @pl.when(inside(OFFSETS[d]))
        def _():
            forward_copy(0, d).start()

    pick_t[...] = one_hot(spread == row_ids)[:, :ghosts]
    doubled = beside([wanted[:, :ghosts]] * 2)
    pick_t2[...] = one_hot(jnp.broadcast_to(doubled, (blocks, 2 * ghosts)) == row_ids)
    part_ref[...] = jnp.zeros_like(part_ref)
    loads[2].wait()
    face_cols = []
    for k in range(faces_n):
        turned = jnp.broadcast_to(faces_ref[k : k + 1, :], (blocks, blocks))
        col = jnp.transpose(turned.astype(F32)).astype(jnp.int32)
        face_cols.append(col)
        p_own[k * blocks : (k + 1) * blocks, :] = one_hot(col == lane_ids)
        pt_own[k * blocks : (k + 1) * blocks, :] = one_hot(turned == row_ids)
        hit = one_hot(turned[:ghosts] == row_ids[:ghosts] + blocks)
        pt_halo[k * ghosts : (k + 1) * ghosts, :blocks] = hit
        pt_halo[k * ghosts : (k + 1) * ghosts, blocks:] = hit
    for pair in range(faces_n // 2):
        low = lane_ids < ghosts
        col = jnp.where(low, face_cols[2 * pair], face_cols[2 * pair + 1])
        want = jnp.where(low, lane_ids, lane_ids - ghosts) + blocks
        p_halo[:, pair * 2 * ghosts : (pair + 1) * 2 * ghosts] = one_hot(col == want)

    for load in loads[3:]:
        load.wait()
    def picked_rows(value):
        high = value.astype(BF16)
        low = (value - high.astype(F32)).astype(BF16)
        return dot(beside([pick[...], pick[...]]), below([high, low]))

    near_ref[...] = dot(pick[...], p_halo[...]).astype(BF16)
    spot_metric[...] = picked_rows(STEP_SIZE * metric_ref[...])
    for k in range(slots):
        lift_t[:, k * nodes : (k + 1) * nodes] = jnp.transpose(lift_ref[k].astype(F32)).astype(BF16)

    @pl.when(lead)
    def _():
        which = lax.broadcasted_iota(jnp.int32, (levels, nodes), 0)
        angles = jnp.zeros((levels, nodes), F32)
        for n in range(levels):
            angles = jnp.where(which == n, pitch_ref[n], angles)
        turn_ref[0] = jnp.cos(angles)
        turn_ref[1] = jnp.sin(angles)
        back_in[...] = jnp.zeros_like(back_in)
        dup_in[...] = jnp.zeros_like(dup_in)
        four = beside([wanted[:, :ghosts]] * 4)
        ids = lax.broadcasted_iota(jnp.int32, (blocks, 4 * ghosts), 0)
        picks = one_hot(jnp.broadcast_to(four, (blocks, 4 * ghosts)) == ids)
        table = dot(pt_halo[:, :blocks], picks)
        part = lax.broadcasted_iota(jnp.int32, (halo, 4 * ghosts), 1) // ghosts
        for d in DIRS:
            for k in range(faces_n):
                piece = table[k * ghosts + d * halo : k * ghosts + (d + 1) * halo]
                to = (d * faces_n + k) * halo
                et_out[to : to + halo, :] = jnp.where(part == d, piece, 0.0).astype(BF16)
        chosen = dot(pick[...], metric_ref[...].astype(BF16)).astype(BF16)
        for d in DIRS:
            mg_out[d] = chosen[d * halo : (d + 1) * halo]
        for d in DIRS:
            @pl.when(inside(OFFSETS[d]))
            def _():
                metric_copy(d).start()

            @pl.when(inside(-OFFSETS[d]))
            def _():
                table_copy(d).start()

    def factor_copy(level, which):
        ref = (dd_ref, wu_ref)[which]
        return pltpu.make_async_remote_copy(
            src_ref=ref.at[level], dst_ref=ref.at[level], send_sem=factor_sems.at[0, which, level],
            recv_sem=factor_sems.at[1, which, level], device_id=partner, device_id_type=MESH,
        )

    def round_signal(r):
        for side, shift in enumerate((rounds[r], -rounds[r])):
            @pl.when(inside(shift))
            def _():
                pl.semaphore_signal(
                    round_sems.at[r, side], inc=1, device_id=(n_tm - 1, at(shift)), device_id_type=MESH
                )

    def round_wait(r):
        for side, shift in enumerate((rounds[r], -rounds[r])):
            @pl.when(inside(-shift))
            def _():
                pl.semaphore_wait(round_sems.at[r, side], 1)

    def round_step(r):
        if 0 < r <= len(rounds):
            round_wait(r - 1)
        if r < len(rounds):
            round_signal(r)

    def forward(n, carry):
        level = tm * half + n
        active = (n < half - 1) | lead

        @pl.when(n > 0)
        def _():
            for c in range(comps):
                sq_ref[c] = jnp.tanh(u_ref[c]).astype(BF16)

        for r in range(half - 1):
            @pl.when(lead & (n == r + 1))
            def _():
                round_step(r)

        keep = jnp.where(level > 0, 1.0, 0.0).astype(F32)
        for c in range(comps):
            state = u_ref[c]
            t = jnp.tanh(state)
            dd_ref[level, c] = STEP_SIZE * (1.0 - t * t)
            wu_ref[level, c] = (keep * weight_ref[c]) * state

        @pl.when(jnp.logical_not(lead))
        def _():
            factor_copy(level, 0).start()
            factor_copy(level, 1).start()

        @pl.when(level == 1)
        def _():
            cosine, sine = turn_of(0)
            fields = []
            for c in range(comps):
                turning = cosine * src_ref[1, c] - sine * src_ref[0, c]
                fields.append((dd_ref[1, c] * turning).astype(BF16))
            chosen = dot(pick[...], beside(fields)).astype(BF16)
            for d in DIRS:
                for c in range(comps):
                    hint_out[d, c] = chosen[d * halo : (d + 1) * halo, lanes(c)]
            for d in DIRS:
                @pl.when(inside(OFFSETS[d]))
                def _():
                    hint_copy(d).start()

        @pl.when(active)
        def _():
            cosine, sine = turn_of(level)
            squashed = beside(sq_ref[c] for c in range(comps))
            for k in range(slots):
                if k == 0:
                    stacked = sq_ref[...].reshape(comps * blocks, nodes)
                else:
                    got = dot(p_own[(k - 1) * blocks : k * blocks, :], squashed).astype(BF16)
                    stacked = below(got[:, lanes(c)] for c in range(comps))
                y_ref[k] = dot(stacked, lift_t[:, lanes(k)])

            def own_mix(r, carry):
                start = pl.multiple_of(r * chunk, chunk)
                metric_half = STEP_SIZE * metric_ref[pl.ds(start, chunk), :]
                sums = [None] * comps
                for k in range(slots):
                    for c in range(comps):
                        term = y_ref[k, pl.ds(c * blocks + start, chunk), :]
                        for e in range(comps):
                            add = coef(k, e, c) * term
                            sums[e] = add if sums[e] is None else sums[e] + add
                for e in range(comps):
                    rows = pl.ds(start, chunk)
                    forcing = cosine * src_ref[0, e, rows, :] + sine * src_ref[1, e, rows, :]
                    base_ref[e, rows, :] = u_ref[e, rows, :] + STEP_SIZE * forcing - metric_half * sums[e]
                return carry

            lax.fori_loop(0, blocks // chunk, own_mix, 0)
            spot_base[...] = picked_rows(beside(base_ref[e] for e in range(comps)))

            for d in DIRS:
                @pl.when(inside(OFFSETS[d]))
                def _():
                    forward_copy(n, d).wait_send()

            for d in DIRS:
                @pl.when(inside(-OFFSETS[d]))
                def _():
                    forward_copy(n, d).wait_recv()

            stacked = below(ghost_rows(in_buf, (level,), c) for c in range(comps))
            yh_ref[...] = dot(stacked, lift_t[:, nodes:])
            for k in range(1, slots):
                for part in range(ghosts // chunk):
                    for e in range(comps):
                        total = None
                        for c in range(comps):
                            row = c * ghosts + part * chunk
                            add = coef(k, e, c) * yh_ref[row : row + chunk, lanes(k - 1)]
                            total = add if total is None else total + add
                        row = (k - 1) * ghosts + part * chunk
                        z_ref[e, row : row + chunk, :] = total.astype(BF16)
            later = n + 1

            @pl.when(later < half)
            def _():
                more = dot(near_ref[...], beside(z_ref[e] for e in range(comps)))
                for c in range(comps):
                    spot = spot_base[:, lanes(c)] - spot_metric[...] * more[:, lanes(c)]
                    value = jnp.tanh(spot).astype(BF16)
                    for d in DIRS:
                        out_buf[later, d, c] = value[d * halo : (d + 1) * halo]
                for d in DIRS:
                    @pl.when(inside(OFFSETS[d]) & ((later < half - 1) | lead))
                    def _():
                        forward_copy(later, d).start()

                    @pl.when(inside(OFFSETS[d]) & jnp.logical_not(lead) & (lax.rem(later, 2) == 1))
                    def _():
                        ghost_copy(later, d).start()

            more = dot(p_halo[...], beside(z_ref[e] for e in range(comps)))
            half_metric = STEP_SIZE * metric_ref[...]
            for e in range(comps):
                u_ref[e] = base_ref[e] - half_metric * more[:, lanes(e)]

        return carry

    lax.fori_loop(0, half, forward, 0)

    def hand_copy(c):
        return pltpu.make_async_remote_copy(
            src_ref=a_ref.at[c], dst_ref=out_ref.at[0, c], send_sem=hand_sems.at[0, c], recv_sem=hand_sems.at[1, c],
            device_id=partner, device_id_type=MESH,
        )

    def keep_copy():
        return pltpu.make_async_copy(hand_ref, out_ref.at[0], keep_sems)

    def grad_copy(source, other):
        return pltpu.make_async_remote_copy(
            src_ref=row_ref, dst_ref=rows_ref.at[source], send_sem=gsend_sems.at[other],
            recv_sem=grecv_sems.at[source], device_id=(other // n_space, lax.rem(other, n_space)),
            device_id_type=MESH,
        )

    def mix_back(k, row, rows, to):
        for c in range(comps):
            total = None
            for e in range(comps):
                add = coef(k, e, c) * gw_ref[row : row + rows, lanes(e)]
                total = add if total is None else total + add
            gh_ref[k - 1, c * ghosts + to : c * ghosts + to + rows, :] = total.astype(BF16)

    def lift_back():
        return dot(beside(gh_ref[k] for k in range(faces_n)), lift_ref[1:].reshape(faces_n * nodes, nodes))

    def halo_part(ref, level, keep):
        for e in range(comps):
            w = metric_ref[...] * ref[e]
            if keep:
                wf_ref[e] = w
            high = w.astype(BF16)
            split_ref[e, :blocks, :] = high
            split_ref[e, blocks:, :] = (w - high.astype(F32)).astype(BF16)
        gw_ref[...] = dot(pt_halo[...], beside(split_ref[e] for e in range(comps)))
        for k in range(1, slots):
            for part in range(ghosts // chunk):
                mix_back(k, (k - 1) * ghosts + part * chunk, chunk, part * chunk)
        lifted = lift_back().astype(BF16)
        for d in DIRS:
            for c in range(comps):
                row = c * ghosts + d * halo
                back_out[level, d, c] = lifted[row : row + halo]
        for d in DIRS:
            @pl.when(inside(-OFFSETS[d]))
            def _():
                backward_copy(level, d).start()

    def own_mixing():
        for k in [*range(1, slots), 0]:
            for r in range(blocks // chunk):
                rows = slice(r * chunk, (r + 1) * chunk)
                weighted = [wf_ref[e, rows, :] for e in range(comps)]
                for c in range(comps):
                    total = None
                    for e in range(comps):
                        add = coef(k, e, c) * weighted[e]
                        total = add if total is None else total + add
                    if k == 0:
                        g_ref[0, c * blocks + r * chunk : c * blocks + (r + 1) * chunk, :] = total.astype(BF16)
                    else:
                        mixed_ref[k - 1, c, rows, :] = total.astype(BF16)
            if k > 0:
                wide = beside(mixed_ref[k - 1, c] for c in range(comps))
                got = dot(pt_own[(k - 1) * blocks : k * blocks, :], wide).astype(BF16)
                for c in range(comps):
                    g_ref[k, c * blocks : (c + 1) * blocks, :] = got[:, lanes(c)]

    def own_lift(level):
        pushed = dot(beside(g_ref[k] for k in range(slots)), lift_ref[...].reshape(slots * nodes, nodes))
        for c in range(comps):
            base_ref[c] = a_ref[c] + wu_ref[level, c] - dd_ref[level, c] * pushed[c * blocks : (c + 1) * blocks]

    def add_grad(level, ref=a_ref, extra=None):
        cosine, sine = turn_ref[0, pl.ds(level, 1), :], turn_ref[1, pl.ds(level, 1), :]
        sums = extra
        for e in range(comps):
            part = ref[e] * (cosine * src_ref[1, e] - sine * src_ref[0, e])
            sums = part if sums is None else sums + part
        part_ref[pl.ds(level, 1), :] = jnp.sum(sums, axis=0, keepdims=True)

    def total_grad():
        values = jnp.sum(part_ref[...], axis=1, keepdims=True) * (STEP_SIZE / norm)
        spots = lax.broadcasted_iota(jnp.int32, (levels, nodes), 1)
        own = lax.broadcasted_iota(jnp.int32, (levels, nodes), 0)
        row_ref[...] = jnp.sum(jnp.where(spots == own, values, 0.0), axis=0, keepdims=True)

    def backward(j, carry):
        high = levels - 1 - 2 * j
        low = high - 1

        halo_part(a_ref, high, True)

        @pl.when(j == 0)
        def _():
            for d in DIRS:
                @pl.when(inside(-OFFSETS[d]))
                def _():
                    metric_copy(d).wait_recv()

        @pl.when(high < half)
        def _():
            for d in DIRS:
                @pl.when(inside(-OFFSETS[d]))
                def _():
                    ghost_copy(high, d).wait_recv()

            for which in range(2):
                factor_copy(high, which).wait_recv()
                factor_copy(low, which).wait_recv()

        for far in DIRS:
            spread_metric = mg_in[far].astype(F32)
            d = OFFSETS.index(-OFFSETS[far])
            for c in range(comps):
                t = in_buf[high, far, c].astype(F32)
                factor = spread_metric * (STEP_SIZE - STEP_SIZE * t * t)
                scaled = (factor * back_out[high, far, c].astype(F32)).astype(BF16)
                dup_out[j, far, c] = scaled
                dup_in[j, d, far, c] = scaled
        for d, far in second_pairs:
            @pl.when(inside(-OFFSETS[far]) & inside(-OFFSETS[far] - OFFSETS[d]))
            def _():
                second_copy(j, d, far).start()

        add_grad(high)
        own_mixing()
        own_lift(high)
        halo_part(base_ref, low, False)

        @pl.when(low == 0)
        def _():
            for d in DIRS:
                @pl.when(inside(-OFFSETS[d]))
                def _():
                    hint_copy(d).wait_recv()

            missing = None
            for d in DIRS:
                for c in range(comps):
                    part = back_out[high, d, c].astype(F32) * hint_in[d, c].astype(F32)
                    missing = part if missing is None else missing + part
            add_grad(low, base_ref, below([-missing, jnp.zeros((blocks - halo, nodes), F32)]))
            total_grad()

            def tell(r, carry):
                other = lax.rem(me + r, n_dev)
                grad_copy(sp, other).start()
                return carry

            lax.fori_loop(1, n_dev, tell, 0)

        for d in DIRS:
            @pl.when(inside(OFFSETS[d]))
            def _():
                backward_copy(high, d).wait_recv()

        more = dot(pick_t[...], ghost_wide(back_in, (high,)))
        for c in range(comps):
            state = base_ref[c] - dd_ref[high, c] * more[:, lanes(c)]
            a_ref[c] = state
            wf_ref[c] = metric_ref[...] * state

        add_grad(low)

        own_mixing()
        own_lift(low)

        @pl.when(j == 0)
        def _():
            for d in DIRS:
                @pl.when(inside(OFFSETS[d]))
                def _():
                    table_copy(d).wait_recv()

        for d, far in second_pairs:
            @pl.when(inside(OFFSETS[d]) & inside(OFFSETS[d] + OFFSETS[far]))
            def _():
                second_copy(j, d, far).wait_recv()

        rows = [below(dup_in[j, d, far, c] for d in DIRS for far in DIRS) for c in range(comps)]
        gw_ref[...] = dot(et_in[...], beside(rows))
        for k in range(1, slots):
            for d in DIRS:
                mix_back(k, (d * faces_n + k - 1) * halo, halo, d * halo)
        lifted = (-lift_back()).astype(BF16)
        for c in range(comps):
            last_ref[c] = lifted[c * ghosts : (c + 1) * ghosts]

        for d in DIRS:
            @pl.when(inside(OFFSETS[d]))
            def _():
                backward_copy(low, d).wait_recv()

        late = beside(below([ghost_rows(back_in, (low,), c), last_ref[c]]) for c in range(comps))
        more = dot(pick_t2[...], late)
        for c in range(comps):
            a_ref[c] = base_ref[c] - dd_ref[low, c] * more[:, lanes(c)]

        @pl.when(low == half)
        def _():
            for c in range(comps):
                hand_ref[c] = a_ref[c]
            keep_copy().start()

        return carry

    @pl.when(lead)
    def _():
        for r in range(half - 1, len(rounds) + 1):
            round_step(r)
        for c in range(comps):
            a_ref[c] = a_ref[c] + weight_ref[c] * u_ref[c]
        lax.fori_loop(0, levels // 2, backward, 0)
        for c in range(comps):
            hand_copy(c).start()
        rows_ref[sp] = row_ref[...]

        def drained(j, carry):
            for d, far in second_pairs:
                @pl.when(inside(-OFFSETS[far]) & inside(-OFFSETS[far] - OFFSETS[d]))
                def _():
                    second_copy(j, d, far).wait_send()
            for d in DIRS:
                @pl.when(inside(-OFFSETS[d]))
                def _():
                    backward_copy(2 * j, d).wait_send()
                    backward_copy(2 * j + 1, d).wait_send()
            return carry

        lax.fori_loop(0, levels // 2, drained, 0)
        for d in DIRS:
            @pl.when(inside(OFFSETS[d]))
            def _():
                metric_copy(d).wait_send()

            @pl.when(inside(-OFFSETS[d]))
            def _():
                table_copy(d).wait_send()

        def settle(r, carry):
            other = lax.rem(sp + r, n_space)
            grad_copy(other, me).wait_recv()
            return carry

        lax.fori_loop(1, n_space, settle, 0)

    @pl.when(jnp.logical_not(lead))
    def _():
        def settle(r, carry):
            grad_copy(r, me).wait_recv()
            return carry

        lax.fori_loop(0, n_space, settle, 0)

    grad_ref[...] = jnp.sum(rows_ref[...], axis=0)[0, : grad_ref.shape[0]]

    @pl.when(lead)
    def _():
        for c in range(comps):
            hand_copy(c).wait_send()
        keep_copy().wait()

        def sent(r, carry):
            grad_copy(sp, lax.rem(me + r, n_dev)).wait_send()
            return carry

        lax.fori_loop(1, n_dev, sent, 0)

    @pl.when(jnp.logical_not(lead))
    def _():
        for c in range(comps):
            hand_copy(c).wait_recv()
        for level in range(half):
            factor_copy(level, 0).wait_send()
            factor_copy(level, 1).wait_send()
        for d in DIRS:
            @pl.when(inside(OFFSETS[d]))
            def _():
                hint_copy(d).wait_send()
                for level in range(1, half, 2):
                    ghost_copy(level, d).wait_send()


def finish_kernel(pieces, held_hbm, grad_hbm, out_hbm, grad_out, buf, row, sems):
    inward = [pltpu.make_async_copy(held_hbm.at[0, c], buf.at[c], sems.at[0, c]) for c in range(pieces)]
    outward = [pltpu.make_async_copy(buf.at[c], out_hbm.at[0, c], sems.at[1, c]) for c in range(pieces)]
    inward.append(pltpu.make_async_copy(grad_hbm, row, sems.at[0, pieces]))
    outward.append(pltpu.make_async_copy(row, grad_out, sems.at[1, pieces]))
    for copy in inward:
        copy.start()
    for first, second in zip(inward, outward):
        first.wait()
        second.start()
    for copy in outward:
        copy.wait()


def shards(
    checkpoints, sources, pitch, metric, obj_weight, adjoint_end, lift, mixing, faces, send_idx
):
    comps = sources.shape[1]
    blocks, nodes = metric.shape
    slots = lift.shape[0]
    faces_n = slots - 1
    halo = send_idx.shape[2]
    n_tm = lax.axis_size("tm")
    n_space = lax.axis_size("space")
    levels = pitch.shape[0]
    half = levels // n_tm
    twos = levels // 2
    ghosts = 4 * halo
    norm = math.sqrt(comps * nodes * blocks * n_space)
    wide = comps * nodes
    field = (comps, blocks, nodes)
    group = (4, comps, halo, nodes)
    vmem = pl.BlockSpec(memory_space=pltpu.VMEM)
    anym = pl.BlockSpec(memory_space=pl.ANY)
    dma = pltpu.SemaphoreType.DMA
    n_dev = n_tm * n_space
    dims = (comps, blocks, nodes, slots, halo, half, n_tm, n_space, norm)
    bounds, grad = pl.pallas_call(
        functools.partial(window_kernel, dims),
        out_shape=(
            jax.ShapeDtypeStruct((1, *field), F32),
            jax.ShapeDtypeStruct((levels,), F32),
        ),
        in_specs=[anym] * 10,
        out_specs=(anym, vmem),
        scratch_shapes=[
            pltpu.SMEM(pitch.shape, F32),
            pltpu.SMEM(mixing.shape, F32),
            pltpu.VMEM(field, F32),
            pltpu.VMEM(lift.shape, BF16),
            pltpu.VMEM(faces.shape[::-1], jnp.int32),
            pltpu.VMEM(send_idx.shape, jnp.int32),
            pltpu.VMEM((2, *field), F32),
            pltpu.VMEM((blocks, nodes), F32),
            pltpu.VMEM(field, F32),
            pltpu.VMEM(field, F32),
            pltpu.VMEM(field, F32),
            pltpu.VMEM(field, F32),
            pltpu.VMEM((levels, *field), F32),
            pltpu.VMEM((levels, *field), F32),
            pltpu.VMEM((nodes, slots * nodes), BF16),
            pltpu.VMEM(field, BF16),
            pltpu.VMEM((faces_n * blocks, blocks), BF16),
            pltpu.VMEM((blocks, faces_n * ghosts), BF16),
            pltpu.VMEM((faces_n * blocks, blocks), BF16),
            pltpu.VMEM((faces_n * ghosts, 2 * blocks), BF16),
            pltpu.VMEM((ghosts, blocks), BF16),
            pltpu.VMEM((blocks, ghosts), BF16),
            pltpu.VMEM((blocks, 2 * ghosts), BF16),
            pltpu.VMEM((half, *group), BF16),
            pltpu.VMEM((levels, *group), BF16),
            pltpu.VMEM((levels, *group), BF16),
            pltpu.VMEM((levels, *group), BF16),
            pltpu.VMEM((slots, comps * blocks, nodes), F32),
            pltpu.VMEM((comps * ghosts, faces_n * nodes), F32),
            pltpu.VMEM((comps, faces_n * ghosts, nodes), BF16),
            pltpu.VMEM((faces_n, *field), BF16),
            pltpu.VMEM((slots, comps * blocks, nodes), BF16),
            pltpu.VMEM((faces_n * ghosts, wide), F32),
            pltpu.VMEM((faces_n, comps * ghosts, nodes), BF16),
            pltpu.VMEM((comps, 2 * blocks, nodes), BF16),
            pltpu.VMEM(field, F32),
            pltpu.VMEM((1, nodes), F32),
            pltpu.VMEM((n_space, 1, nodes), F32),
            pltpu.VMEM((faces_n * ghosts, 4 * ghosts), BF16),
            pltpu.VMEM((faces_n * ghosts, 4 * ghosts), BF16),
            pltpu.VMEM((4, halo, nodes), BF16),
            pltpu.VMEM((4, halo, nodes), BF16),
            pltpu.VMEM((twos, *group), BF16),
            pltpu.VMEM((twos, 4, *group), BF16),
            pltpu.VMEM((comps, ghosts, nodes), BF16),
            pltpu.VMEM((2, levels, nodes), F32),
            pltpu.VMEM((levels, nodes), F32),
            pltpu.VMEM(group, BF16),
            pltpu.VMEM(group, BF16),
            pltpu.VMEM((ghosts, faces_n * ghosts), BF16),
            pltpu.VMEM((ghosts, nodes), F32),
            pltpu.VMEM((ghosts, wide), F32),
            dma((10,)),
            dma((half, 4)),
            dma((half, 4)),
            dma((levels, 4)),
            dma((levels, 4)),
            dma((2, comps)),
            dma((2, 2, half)),
            dma((n_dev,)),
            dma((n_space,)),
            dma((2, 4)),
            dma((2, 4)),
            dma((2, half // 2, 4)),
            dma((twos, 16)),
            dma((twos, 16)),
            pltpu.SemaphoreType.REGULAR((max(1, len(rounds_of(n_space))), 2)),
            dma((2, 4)),
            dma(()),
        ],
        compiler_params=pltpu.CompilerParams(
            collective_id=0, has_side_effects=True, vmem_limit_bytes=60 * 1024 * 1024
        ),
        name="window",
    )(pitch, mixing, checkpoints, sources, metric, obj_weight, adjoint_end, lift, faces.T, send_idx)
    return pl.pallas_call(
        functools.partial(finish_kernel, comps),
        out_shape=(
            jax.ShapeDtypeStruct((1, *field), F32),
            jax.ShapeDtypeStruct((levels,), F32),
        ),
        in_specs=[anym] * 2,
        out_specs=(anym, anym),
        scratch_shapes=[pltpu.VMEM(field, F32), pltpu.VMEM((levels,), F32), dma((2, comps + 1))],
        compiler_params=pltpu.CompilerParams(vmem_limit_bytes=60 * 1024 * 1024),
        name="finish",
    )(bounds, grad)


def solution(mesh):
    placed = (
        P("tm", None, "space", None),
        P(None, None, "space", None),
        P(),
        P("space", None),
        P(None, "space", None),
        P(None, "space", None),
        P(),
        P(),
        P("space", None),
        P("space", None, None),
    )
    return jax.shard_map(
        shards,
        mesh=mesh,
        in_specs=placed,
        out_specs=(P("tm", None, "space", None), P()),
        check_vma=False,
    )
```

```python
import functools
import math

import jax
import jax.numpy as jnp
from jax import lax
from jax.experimental import pallas as pl
from jax.experimental.pallas import tpu as pltpu
from jax.sharding import PartitionSpec as P

OFFSETS = (1, -1, 2, -2)
STEP_SIZE = 0.5
F32 = jnp.float32
BF16 = jnp.bfloat16
MESH = pl.DeviceIdType.MESH
DIRS = range(4)


def dot(a, b):
    return jnp.dot(a, b, preferred_element_type=F32)


def one_hot(hit):
    return hit.astype(F32).astype(BF16)


def beside(parts):
    return jnp.concatenate(list(parts), axis=1)


def below(parts):
    return jnp.concatenate(list(parts), axis=0)


def rounds_of(n_space):
    reach, rounds = 2 * max(OFFSETS), []
    while reach < n_space - 1:
        rounds.append(reach)
        reach *= 2
    return rounds


def window_kernel(
    dims,
    pitch_hbm, mixing_hbm, cp_hbm, src_hbm, metric_hbm, weight_hbm, end_hbm, lift_hbm, faces_hbm, send_hbm,
    out_ref, grad_ref,
    pitch_ref, mixing_ref, u_ref, lift_ref, faces_ref, send_ref, src_ref, metric_ref, weight_ref, a_ref, hand_ref,
    base_ref, dd_ref, wu_ref, lift_t, sq_ref,
    p_own, p_halo, pt_own, pt_halo, pick, pick_t, pick_t2, out_buf, in_buf, back_out, back_in, y_ref, yh_ref, z_ref,
    mixed_ref, g_ref, gw_ref, gh_ref, split_ref, wf_ref, row_ref, rows_ref,
    et_out, et_in, mg_out, mg_in, dup_out, dup_in, last_ref, turn_ref, part_ref, hint_out, hint_in, near_ref, spot_metric, spot_base, scale_ref,
    load_sems, send_sems, recv_sems, bsend_sems, brecv_sems, hand_sems, factor_sems, gsend_sems, grecv_sems,
    table_sems, metric_sems, ghost_sems, dsend_sems, drecv_sems, round_sems, hint_sems, keep_sems,
):
    comps, blocks, nodes, slots, halo, half, n_tm, n_space, norm = dims
    ghosts = 4 * halo
    faces_n = slots - 1
    tm = lax.axis_index("tm")
    sp = lax.axis_index("space")
    n_dev = n_tm * n_space
    me = tm * n_space + sp
    lead = tm == n_tm - 1
    partner = (n_tm - 1 - tm, sp)
    levels = half * n_tm
    rounds = rounds_of(n_space)
    chunk = 32

    pairs = [
        (send_hbm, send_ref),
        (cp_hbm.at[0], u_ref),
        (faces_hbm, faces_ref),
        (pitch_hbm, pitch_ref),
        (mixing_hbm, mixing_ref),
        (lift_hbm, lift_ref),
        (metric_hbm, metric_ref),
        (weight_hbm, weight_ref),
        (src_hbm, src_ref),
        (end_hbm, a_ref),
    ]
    loads = [pltpu.make_async_copy(src, dst, load_sems.at[i]) for i, (src, dst) in enumerate(pairs)]
    for load in loads:
        load.start()

    in_buf[...] = jnp.zeros_like(in_buf)

    @pl.when(lead)
    def _():
        et_in[...] = jnp.zeros_like(et_in)
        mg_in[...] = jnp.zeros_like(mg_in)
        hint_in[...] = jnp.zeros_like(hint_in)

    barrier = pltpu.get_barrier_semaphore()

    def inside(shift):
        return (sp + shift >= 0) & (sp + shift < n_space)

    def at(shift):
        return jnp.clip(sp + shift, 0, n_space - 1)

    met = n_tm - 1
    pl.semaphore_signal(barrier, inc=1, device_id=partner, device_id_type=MESH)
    for shift in OFFSETS:
        met = met + n_tm * inside(shift).astype(jnp.int32)

        @pl.when(inside(shift))
        def _():
            for side in range(n_tm):
                pl.semaphore_signal(barrier, inc=1, device_id=(side, at(shift)), device_id_type=MESH)

    def lanes(c):
        return slice(c * nodes, (c + 1) * nodes)

    def target(shift):
        return (tm, at(shift))

    def forward_copy(n, d):
        return pltpu.make_async_remote_copy(
            src_ref=out_buf.at[n, d], dst_ref=in_buf.at[tm * half + n, d],
            send_sem=send_sems.at[n, d], recv_sem=recv_sems.at[n, d],
            device_id=target(OFFSETS[d]), device_id_type=MESH,
        )

    def ghost_copy(n, d):
        return pltpu.make_async_remote_copy(
            src_ref=out_buf.at[n, d], dst_ref=in_buf.at[n, d],
            send_sem=ghost_sems.at[0, n // 2, d], recv_sem=ghost_sems.at[1, n // 2, d],
            device_id=(n_tm - 1, at(OFFSETS[d])), device_id_type=MESH,
        )

    def hint_copy(d):
        return pltpu.make_async_remote_copy(
            src_ref=hint_out.at[d], dst_ref=hint_in.at[d],
            send_sem=hint_sems.at[0, d], recv_sem=hint_sems.at[1, d],
            device_id=(n_tm - 1, at(OFFSETS[d])), device_id_type=MESH,
        )

    def metric_copy(d):
        return pltpu.make_async_remote_copy(
            src_ref=mg_out.at[d], dst_ref=mg_in.at[d],
            send_sem=metric_sems.at[0, d], recv_sem=metric_sems.at[1, d],
            device_id=target(OFFSETS[d]), device_id_type=MESH,
        )

    def table_copy(d):
        rows = pl.ds(d * faces_n * halo, faces_n * halo)
        return pltpu.make_async_remote_copy(
            src_ref=et_out.at[rows], dst_ref=et_in.at[rows],
            send_sem=table_sems.at[0, d], recv_sem=table_sems.at[1, d],
            device_id=target(-OFFSETS[d]), device_id_type=MESH,
        )

    def second_copy(slot, d, far):
        return pltpu.make_async_remote_copy(
            src_ref=dup_out.at[slot, far], dst_ref=dup_in.at[slot, d, far],
            send_sem=dsend_sems.at[slot, 4 * d + far], recv_sem=drecv_sems.at[slot, 4 * d + far],
            device_id=target(-OFFSETS[far] - OFFSETS[d]), device_id_type=MESH,
        )

    second_pairs = [(d, far) for d in DIRS for far in DIRS if OFFSETS[d] + OFFSETS[far] != 0]
    second_pairs = sorted(second_pairs, key=lambda p: -abs(OFFSETS[p[0]] + OFFSETS[p[1]]))

    def backward_copy(n, d):
        return pltpu.make_async_remote_copy(
            src_ref=back_out.at[n, d], dst_ref=back_in.at[n, d],
            send_sem=bsend_sems.at[n, d], recv_sem=brecv_sems.at[n, d],
            device_id=target(-OFFSETS[d]), device_id_type=MESH,
        )

    def coef(k, e, c):
        return mixing_ref[k, e, c]

    def turn_of(level):
        angle = jnp.full((8, nodes), pitch_ref[level], F32)
        return jnp.cos(angle)[0:1], jnp.sin(angle)[0:1]

    def ghost_rows(ref, index, c):
        return below(ref[index + (d, c)] for d in DIRS)

    def ghost_wide(ref, index):
        return beside(ghost_rows(ref, index, c) for c in range(comps))

    def squash_and_pick(n):
        for c in range(comps):
            sq_ref[c] = jnp.tanh(u_ref[c]).astype(BF16)
        picked = dot(pick[...], beside(sq_ref[c] for c in range(comps))).astype(BF16)
        for d in DIRS:
            for c in range(comps):
                out_buf[n, d, c] = picked[d * halo : (d + 1) * halo, lanes(c)]

    row_ids = lax.broadcasted_iota(jnp.int32, (blocks, blocks), 0)
    lane_ids = lax.broadcasted_iota(jnp.int32, (blocks, blocks), 1)
    loads[0].wait()
    wanted = beside(
        [send_ref[0, d : d + 1, :] for d in DIRS] + [jnp.full((1, blocks - ghosts), -1, jnp.int32)]
    )
    spread = jnp.broadcast_to(wanted, (blocks, blocks))
    spread_t = jnp.transpose(spread.astype(F32)).astype(jnp.int32)
    pick[...] = one_hot(spread_t[:ghosts] == lane_ids[:ghosts])
    loads[1].wait()
    squash_and_pick(0)
    pl.semaphore_wait(barrier, met)
    for d in DIRS:
        @pl.when(inside(OFFSETS[d]))
        def _():
            forward_copy(0, d).start()

    pick_t[...] = one_hot(spread == row_ids)[:, :ghosts]
    doubled = beside([wanted[:, :ghosts]] * 2)
    pick_t2[...] = one_hot(jnp.broadcast_to(doubled, (blocks, 2 * ghosts)) == row_ids)
    part_ref[...] = jnp.zeros_like(part_ref)
    loads[2].wait()
    face_cols = []
    for k in range(faces_n):
        turned = jnp.broadcast_to(faces_ref[k : k + 1, :], (blocks, blocks))
        col = jnp.transpose(turned.astype(F32)).astype(jnp.int32)
        face_cols.append(col)
        p_own[k * blocks : (k + 1) * blocks, :] = one_hot(col == lane_ids)
        pt_own[k * blocks : (k + 1) * blocks, :] = one_hot(turned == row_ids)
        hit = one_hot(turned[:ghosts] == row_ids[:ghosts] + blocks)
        pt_halo[k * ghosts : (k + 1) * ghosts, :blocks] = hit
        pt_halo[k * ghosts : (k + 1) * ghosts, blocks:] = hit
    for pair in range(faces_n // 2):
        low = lane_ids < ghosts
        col = jnp.where(low, face_cols[2 * pair], face_cols[2 * pair + 1])
        want = jnp.where(low, lane_ids, lane_ids - ghosts) + blocks
        p_halo[:, pair * 2 * ghosts : (pair + 1) * 2 * ghosts] = one_hot(col == want)

    for load in loads[3:]:
        load.wait()
    def picked_rows(value):
        high = value.astype(BF16)
        low = (value - high.astype(F32)).astype(BF16)
        return dot(beside([pick[...], pick[...]]), below([high, low]))

    near_ref[...] = dot(pick[...], p_halo[...]).astype(BF16)
    spot_metric[...] = picked_rows(STEP_SIZE * metric_ref[...])
    for k in range(slots):
        lift_t[:, k * nodes : (k + 1) * nodes] = jnp.transpose(lift_ref[k].astype(F32)).astype(BF16)

    @pl.when(lead)
    def _():
        which = lax.broadcasted_iota(jnp.int32, (levels, nodes), 0)
        angles = jnp.zeros((levels, nodes), F32)
        for n in range(levels):
            angles = jnp.where(which == n, pitch_ref[n], angles)
        turn_ref[0] = jnp.cos(angles)
        turn_ref[1] = jnp.sin(angles)
        back_in[...] = jnp.zeros_like(back_in)
        dup_in[...] = jnp.zeros_like(dup_in)
        four = beside([wanted[:, :ghosts]] * 4)
        ids = lax.broadcasted_iota(jnp.int32, (blocks, 4 * ghosts), 0)
        picks = one_hot(jnp.broadcast_to(four, (blocks, 4 * ghosts)) == ids)
        table = dot(pt_halo[:, :blocks], picks)
        part = lax.broadcasted_iota(jnp.int32, (halo, 4 * ghosts), 1) // ghosts
        for d in DIRS:
            for k in range(faces_n):
                piece = table[k * ghosts + d * halo : k * ghosts + (d + 1) * halo]
                to = (d * faces_n + k) * halo
                et_out[to : to + halo, :] = jnp.where(part == d, piece, 0.0).astype(BF16)
        chosen = dot(pick[...], metric_ref[...].astype(BF16)).astype(BF16)
        for d in DIRS:
            mg_out[d] = chosen[d * halo : (d + 1) * halo]
        for d in DIRS:
            @pl.when(inside(OFFSETS[d]))
            def _():
                metric_copy(d).start()

            @pl.when(inside(-OFFSETS[d]))
            def _():
                table_copy(d).start()

    def factor_copy(level, which):
        ref = (dd_ref, wu_ref)[which]
        return pltpu.make_async_remote_copy(
            src_ref=ref.at[level], dst_ref=ref.at[level], send_sem=factor_sems.at[0, which, level],
            recv_sem=factor_sems.at[1, which, level], device_id=partner, device_id_type=MESH,
        )

    def round_signal(r):
        for side, shift in enumerate((rounds[r], -rounds[r])):
            @pl.when(inside(shift))
            def _():
                pl.semaphore_signal(
                    round_sems.at[r, side], inc=1, device_id=(n_tm - 1, at(shift)), device_id_type=MESH
                )

    def round_wait(r):
        for side, shift in enumerate((rounds[r], -rounds[r])):
            @pl.when(inside(-shift))
            def _():
                pl.semaphore_wait(round_sems.at[r, side], 1)

    def round_step(r):
        if 0 < r <= len(rounds):
            round_wait(r - 1)
        if r < len(rounds):
            round_signal(r)

    def forward(n, carry):
        level = tm * half + n
        active = (n < half - 1) | lead

        @pl.when(n > 0)
        def _():
            for c in range(comps):
                sq_ref[c] = jnp.tanh(u_ref[c]).astype(BF16)

        for r in range(half - 1):
            @pl.when(lead & (n == r + 1))
            def _():
                round_step(r)

        keep = jnp.where(level > 0, 1.0, 0.0).astype(F32)
        for c in range(comps):
            state = u_ref[c]
            t = jnp.tanh(state)
            dd_ref[level, c] = STEP_SIZE * (1.0 - t * t)
            wu_ref[level, c] = (keep * weight_ref[c]) * state

        @pl.when(jnp.logical_not(lead))
        def _():
            factor_copy(level, 0).start()
            factor_copy(level, 1).start()

        @pl.when(level == 1)
        def _():
            cosine, sine = turn_of(0)
            fields = []
            for c in range(comps):
                turning = cosine * src_ref[1, c] - sine * src_ref[0, c]
                fields.append((dd_ref[1, c] * turning).astype(BF16))
            chosen = dot(pick[...], beside(fields)).astype(BF16)
            for d in DIRS:
                for c in range(comps):
                    hint_out[d, c] = chosen[d * halo : (d + 1) * halo, lanes(c)]
            for d in DIRS:
                @pl.when(inside(OFFSETS[d]))
                def _():
                    hint_copy(d).start()

        @pl.when(active)
        def _():
            cosine, sine = turn_of(level)
            squashed = beside(sq_ref[c] for c in range(comps))
            for k in range(slots):
                if k == 0:
                    stacked = sq_ref[...].reshape(comps * blocks, nodes)
                else:
                    got = dot(p_own[(k - 1) * blocks : k * blocks, :], squashed).astype(BF16)
                    stacked = below(got[:, lanes(c)] for c in range(comps))
                y_ref[k] = dot(stacked, lift_t[:, lanes(k)])

            def own_mix(r, carry):
                start = pl.multiple_of(r * chunk, chunk)
                metric_half = STEP_SIZE * metric_ref[pl.ds(start, chunk), :]
                sums = [None] * comps
                for k in range(slots):
                    for c in range(comps):
                        term = y_ref[k, pl.ds(c * blocks + start, chunk), :]
                        for e in range(comps):
                            add = coef(k, e, c) * term
                            sums[e] = add if sums[e] is None else sums[e] + add
                for e in range(comps):
                    rows = pl.ds(start, chunk)
                    forcing = cosine * src_ref[0, e, rows, :] + sine * src_ref[1, e, rows, :]
                    base_ref[e, rows, :] = u_ref[e, rows, :] + STEP_SIZE * forcing - metric_half * sums[e]
                return carry

            lax.fori_loop(0, blocks // chunk, own_mix, 0)
            spot_base[...] = picked_rows(beside(base_ref[e] for e in range(comps)))

            for d in DIRS:
                @pl.when(inside(OFFSETS[d]))
                def _():
                    forward_copy(n, d).wait_send()

            for d in DIRS:
                @pl.when(inside(-OFFSETS[d]))
                def _():
                    forward_copy(n, d).wait_recv()

            stacked = below(ghost_rows(in_buf, (level,), c) for c in range(comps))
            yh_ref[...] = dot(stacked, lift_t[:, nodes:])
            for k in range(1, slots):
                for part in range(ghosts // chunk):
                    for e in range(comps):
                        total = None
                        for c in range(comps):
                            row = c * ghosts + part * chunk
                            add = coef(k, e, c) * yh_ref[row : row + chunk, lanes(k - 1)]
                            total = add if total is None else total + add
                        row = (k - 1) * ghosts + part * chunk
                        z_ref[e, row : row + chunk, :] = total.astype(BF16)
            later = n + 1

            @pl.when(later < half)
            def _():
                more = dot(near_ref[...], beside(z_ref[e] for e in range(comps)))
                for c in range(comps):
                    spot = spot_base[:, lanes(c)] - spot_metric[...] * more[:, lanes(c)]
                    value = jnp.tanh(spot).astype(BF16)
                    for d in DIRS:
                        out_buf[later, d, c] = value[d * halo : (d + 1) * halo]
                for d in DIRS:
                    @pl.when(inside(OFFSETS[d]) & ((later < half - 1) | lead))
                    def _():
                        forward_copy(later, d).start()

                    @pl.when(inside(OFFSETS[d]) & jnp.logical_not(lead) & (lax.rem(later, 2) == 1))
                    def _():
                        ghost_copy(later, d).start()

            more = dot(p_halo[...], beside(z_ref[e] for e in range(comps)))
            half_metric = STEP_SIZE * metric_ref[...]
            for e in range(comps):
                u_ref[e] = base_ref[e] - half_metric * more[:, lanes(e)]

        return carry

    lax.fori_loop(0, half, forward, 0)

    def hand_copy(c):
        return pltpu.make_async_remote_copy(
            src_ref=a_ref.at[c], dst_ref=out_ref.at[0, c], send_sem=hand_sems.at[0, c], recv_sem=hand_sems.at[1, c],
            device_id=partner, device_id_type=MESH,
        )

    def keep_copy():
        return pltpu.make_async_copy(hand_ref, out_ref.at[0], keep_sems)

    def grad_copy(source, other):
        return pltpu.make_async_remote_copy(
            src_ref=row_ref, dst_ref=rows_ref.at[source], send_sem=gsend_sems.at[other],
            recv_sem=grecv_sems.at[source], device_id=(other // n_space, lax.rem(other, n_space)),
            device_id_type=MESH,
        )

    def mix_back(k, row, rows, to):
        for c in range(comps):
            total = None
            for e in range(comps):
                add = coef(k, e, c) * gw_ref[row : row + rows, lanes(e)]
                total = add if total is None else total + add
            gh_ref[k - 1, c * ghosts + to : c * ghosts + to + rows, :] = total.astype(BF16)

    def lift_back():
        return dot(beside(gh_ref[k] for k in range(faces_n)), lift_ref[1:].reshape(faces_n * nodes, nodes))

    def prepare(level):
        @pl.when(level < half)
        def _():
            for d in DIRS:
                @pl.when(inside(-OFFSETS[d]))
                def _():
                    ghost_copy(level, d).wait_recv()

            for which in range(2):
                factor_copy(level, which).wait_recv()
                factor_copy(level - 1, which).wait_recv()

        for far in DIRS:
            spread_metric = mg_in[far].astype(F32)
            for c in range(comps):
                t = in_buf[level, far, c].astype(F32)
                scale_ref[far, c] = spread_metric * (STEP_SIZE - STEP_SIZE * t * t)

    def halo_part(ref, level, slot):
        for e in range(comps):
            w = metric_ref[...] * ref[e]
            if slot is not None:
                wf_ref[e] = w
            high = w.astype(BF16)
            split_ref[e, :blocks, :] = high
            split_ref[e, blocks:, :] = (w - high.astype(F32)).astype(BF16)
        gw_ref[...] = dot(pt_halo[...], beside(split_ref[e] for e in range(comps)))
        for k in range(1, slots):
            for part in range(ghosts // chunk):
                mix_back(k, (k - 1) * ghosts + part * chunk, chunk, part * chunk)
        lifted = lift_back()
        for d in DIRS:
            for c in range(comps):
                row = c * ghosts + d * halo
                piece = lifted[row : row + halo]
                back_out[level, d, c] = piece.astype(BF16)
                if slot is not None:
                    scaled = (scale_ref[d, c] * piece).astype(BF16)
                    dup_out[slot, d, c] = scaled
                    dup_in[slot, OFFSETS.index(-OFFSETS[d]), d, c] = scaled
        for d in DIRS:
            @pl.when(inside(-OFFSETS[d]))
            def _():
                backward_copy(level, d).start()
        if slot is not None:
            for d, far in second_pairs:
                @pl.when(inside(-OFFSETS[far]) & inside(-OFFSETS[far] - OFFSETS[d]))
                def _():
                    second_copy(slot, d, far).start()

    def own_mixing():
        for k in [*range(1, slots), 0]:
            for r in range(blocks // chunk):
                rows = slice(r * chunk, (r + 1) * chunk)
                weighted = [wf_ref[e, rows, :] for e in range(comps)]
                for c in range(comps):
                    total = None
                    for e in range(comps):
                        add = coef(k, e, c) * weighted[e]
                        total = add if total is None else total + add
                    if k == 0:
                        g_ref[0, c * blocks + r * chunk : c * blocks + (r + 1) * chunk, :] = total.astype(BF16)
                    else:
                        mixed_ref[k - 1, c, rows, :] = total.astype(BF16)
            if k > 0:
                wide = beside(mixed_ref[k - 1, c] for c in range(comps))
                got = dot(pt_own[(k - 1) * blocks : k * blocks, :], wide).astype(BF16)
                for c in range(comps):
                    g_ref[k, c * blocks : (c + 1) * blocks, :] = got[:, lanes(c)]

    def own_lift(level):
        pushed = dot(beside(g_ref[k] for k in range(slots)), lift_ref[...].reshape(slots * nodes, nodes))
        for c in range(comps):
            base_ref[c] = a_ref[c] + wu_ref[level, c] - dd_ref[level, c] * pushed[c * blocks : (c + 1) * blocks]

    def add_grad(level, ref=a_ref, extra=None):
        cosine, sine = turn_ref[0, pl.ds(level, 1), :], turn_ref[1, pl.ds(level, 1), :]
        sums = extra
        for e in range(comps):
            part = ref[e] * (cosine * src_ref[1, e] - sine * src_ref[0, e])
            sums = part if sums is None else sums + part
        part_ref[pl.ds(level, 1), :] = jnp.sum(sums, axis=0, keepdims=True)

    def total_grad():
        values = jnp.sum(part_ref[...], axis=1, keepdims=True) * (STEP_SIZE / norm)
        spots = lax.broadcasted_iota(jnp.int32, (levels, nodes), 1)
        own = lax.broadcasted_iota(jnp.int32, (levels, nodes), 0)
        row_ref[...] = jnp.sum(jnp.where(spots == own, values, 0.0), axis=0, keepdims=True)

    def backward(j, carry):
        high = levels - 1 - 2 * j
        low = high - 1

        halo_part(a_ref, high, j)
        add_grad(high)
        own_mixing()
        own_lift(high)
        halo_part(base_ref, low, None)

        @pl.when(low > 0)
        def _():
            prepare(high - 2)

        @pl.when(low == 0)
        def _():
            for d in DIRS:
                @pl.when(inside(-OFFSETS[d]))
                def _():
                    hint_copy(d).wait_recv()

            missing = None
            for d in DIRS:
                for c in range(comps):
                    part = back_out[high, d, c].astype(F32) * hint_in[d, c].astype(F32)
                    missing = part if missing is None else missing + part
            add_grad(low, base_ref, below([-missing, jnp.zeros((blocks - halo, nodes), F32)]))
            total_grad()

            def tell(r, carry):
                other = lax.rem(me + r, n_dev)
                grad_copy(sp, other).start()
                return carry

            lax.fori_loop(1, n_dev, tell, 0)

        for d in DIRS:
            @pl.when(inside(OFFSETS[d]))
            def _():
                backward_copy(high, d).wait_recv()

        more = dot(pick_t[...], ghost_wide(back_in, (high,)))
        for c in range(comps):
            state = base_ref[c] - dd_ref[high, c] * more[:, lanes(c)]
            a_ref[c] = state
            wf_ref[c] = metric_ref[...] * state

        add_grad(low)

        own_mixing()
        own_lift(low)

        @pl.when(j == 0)
        def _():
            for d in DIRS:
                @pl.when(inside(OFFSETS[d]))
                def _():
                    table_copy(d).wait_recv()

        for d, far in second_pairs:
            @pl.when(inside(OFFSETS[d]) & inside(OFFSETS[d] + OFFSETS[far]))
            def _():
                second_copy(j, d, far).wait_recv()

        rows = [below(dup_in[j, d, far, c] for d in DIRS for far in DIRS) for c in range(comps)]
        gw_ref[...] = dot(et_in[...], beside(rows))
        for k in range(1, slots):
            for d in DIRS:
                mix_back(k, (d * faces_n + k - 1) * halo, halo, d * halo)
        lifted = (-lift_back()).astype(BF16)
        for c in range(comps):
            last_ref[c] = lifted[c * ghosts : (c + 1) * ghosts]

        for d in DIRS:
            @pl.when(inside(OFFSETS[d]))
            def _():
                backward_copy(low, d).wait_recv()

        late = beside(below([ghost_rows(back_in, (low,), c), last_ref[c]]) for c in range(comps))
        more = dot(pick_t2[...], late)
        for c in range(comps):
            a_ref[c] = base_ref[c] - dd_ref[low, c] * more[:, lanes(c)]

        @pl.when(low == half)
        def _():
            for c in range(comps):
                hand_ref[c] = a_ref[c]
            keep_copy().start()

        return carry

    @pl.when(lead)
    def _():
        for r in range(half - 1, len(rounds) + 1):
            round_step(r)
        for c in range(comps):
            a_ref[c] = a_ref[c] + weight_ref[c] * u_ref[c]
        for d in DIRS:
            @pl.when(inside(-OFFSETS[d]))
            def _():
                metric_copy(d).wait_recv()

        prepare(levels - 1)
        lax.fori_loop(0, levels // 2, backward, 0)
        for c in range(comps):
            hand_copy(c).start()
        rows_ref[sp] = row_ref[...]

        def drained(j, carry):
            for d, far in second_pairs:
                @pl.when(inside(-OFFSETS[far]) & inside(-OFFSETS[far] - OFFSETS[d]))
                def _():
                    second_copy(j, d, far).wait_send()
            for d in DIRS:
                @pl.when(inside(-OFFSETS[d]))
                def _():
                    backward_copy(2 * j, d).wait_send()
                    backward_copy(2 * j + 1, d).wait_send()
            return carry

        lax.fori_loop(0, levels // 2, drained, 0)
        for d in DIRS:
            @pl.when(inside(OFFSETS[d]))
            def _():
                metric_copy(d).wait_send()

            @pl.when(inside(-OFFSETS[d]))
            def _():
                table_copy(d).wait_send()

        def settle(r, carry):
            other = lax.rem(sp + r, n_space)
            grad_copy(other, me).wait_recv()
            return carry

        lax.fori_loop(1, n_space, settle, 0)

    @pl.when(jnp.logical_not(lead))
    def _():
        def settle(r, carry):
            grad_copy(r, me).wait_recv()
            return carry

        lax.fori_loop(0, n_space, settle, 0)

    grad_ref[...] = jnp.sum(rows_ref[...], axis=0)[0, : grad_ref.shape[0]]

    @pl.when(lead)
    def _():
        for c in range(comps):
            hand_copy(c).wait_send()
        keep_copy().wait()

        def sent(r, carry):
            grad_copy(sp, lax.rem(me + r, n_dev)).wait_send()
            return carry

        lax.fori_loop(1, n_dev, sent, 0)

    @pl.when(jnp.logical_not(lead))
    def _():
        for c in range(comps):
            hand_copy(c).wait_recv()
        for level in range(half):
            factor_copy(level, 0).wait_send()
            factor_copy(level, 1).wait_send()
        for d in DIRS:
            @pl.when(inside(OFFSETS[d]))
            def _():
                hint_copy(d).wait_send()
                for level in range(1, half, 2):
                    ghost_copy(level, d).wait_send()


def finish_kernel(pieces, held_hbm, grad_hbm, out_hbm, grad_out, buf, row, sems):
    inward = [pltpu.make_async_copy(held_hbm.at[0, c], buf.at[c], sems.at[0, c]) for c in range(pieces)]
    outward = [pltpu.make_async_copy(buf.at[c], out_hbm.at[0, c], sems.at[1, c]) for c in range(pieces)]
    inward.append(pltpu.make_async_copy(grad_hbm, row, sems.at[0, pieces]))
    outward.append(pltpu.make_async_copy(row, grad_out, sems.at[1, pieces]))
    for copy in inward:
        copy.start()
    for first, second in zip(inward, outward):
        first.wait()
        second.start()
    for copy in outward:
        copy.wait()


def shards(
    checkpoints, sources, pitch, metric, obj_weight, adjoint_end, lift, mixing, faces, send_idx
):
    comps = sources.shape[1]
    blocks, nodes = metric.shape
    slots = lift.shape[0]
    faces_n = slots - 1
    halo = send_idx.shape[2]
    n_tm = lax.axis_size("tm")
    n_space = lax.axis_size("space")
    levels = pitch.shape[0]
    half = levels // n_tm
    twos = levels // 2
    ghosts = 4 * halo
    norm = math.sqrt(comps * nodes * blocks * n_space)
    wide = comps * nodes
    field = (comps, blocks, nodes)
    group = (4, comps, halo, nodes)
    vmem = pl.BlockSpec(memory_space=pltpu.VMEM)
    anym = pl.BlockSpec(memory_space=pl.ANY)
    dma = pltpu.SemaphoreType.DMA
    n_dev = n_tm * n_space
    dims = (comps, blocks, nodes, slots, halo, half, n_tm, n_space, norm)
    bounds, grad = pl.pallas_call(
        functools.partial(window_kernel, dims),
        out_shape=(
            jax.ShapeDtypeStruct((1, *field), F32),
            jax.ShapeDtypeStruct((levels,), F32),
        ),
        in_specs=[anym] * 10,
        out_specs=(anym, vmem),
        scratch_shapes=[
            pltpu.SMEM(pitch.shape, F32),
            pltpu.SMEM(mixing.shape, F32),
            pltpu.VMEM(field, F32),
            pltpu.VMEM(lift.shape, BF16),
            pltpu.VMEM(faces.shape[::-1], jnp.int32),
            pltpu.VMEM(send_idx.shape, jnp.int32),
            pltpu.VMEM((2, *field), F32),
            pltpu.VMEM((blocks, nodes), F32),
            pltpu.VMEM(field, F32),
            pltpu.VMEM(field, F32),
            pltpu.VMEM(field, F32),
            pltpu.VMEM(field, F32),
            pltpu.VMEM((levels, *field), F32),
            pltpu.VMEM((levels, *field), F32),
            pltpu.VMEM((nodes, slots * nodes), BF16),
            pltpu.VMEM(field, BF16),
            pltpu.VMEM((faces_n * blocks, blocks), BF16),
            pltpu.VMEM((blocks, faces_n * ghosts), BF16),
            pltpu.VMEM((faces_n * blocks, blocks), BF16),
            pltpu.VMEM((faces_n * ghosts, 2 * blocks), BF16),
            pltpu.VMEM((ghosts, blocks), BF16),
            pltpu.VMEM((blocks, ghosts), BF16),
            pltpu.VMEM((blocks, 2 * ghosts), BF16),
            pltpu.VMEM((half, *group), BF16),
            pltpu.VMEM((levels, *group), BF16),
            pltpu.VMEM((levels, *group), BF16),
            pltpu.VMEM((levels, *group), BF16),
            pltpu.VMEM((slots, comps * blocks, nodes), F32),
            pltpu.VMEM((comps * ghosts, faces_n * nodes), F32),
            pltpu.VMEM((comps, faces_n * ghosts, nodes), BF16),
            pltpu.VMEM((faces_n, *field), BF16),
            pltpu.VMEM((slots, comps * blocks, nodes), BF16),
            pltpu.VMEM((faces_n * ghosts, wide), F32),
            pltpu.VMEM((faces_n, comps * ghosts, nodes), BF16),
            pltpu.VMEM((comps, 2 * blocks, nodes), BF16),
            pltpu.VMEM(field, F32),
            pltpu.VMEM((1, nodes), F32),
            pltpu.VMEM((n_space, 1, nodes), F32),
            pltpu.VMEM((faces_n * ghosts, 4 * ghosts), BF16),
            pltpu.VMEM((faces_n * ghosts, 4 * ghosts), BF16),
            pltpu.VMEM((4, halo, nodes), BF16),
            pltpu.VMEM((4, halo, nodes), BF16),
            pltpu.VMEM((twos, *group), BF16),
            pltpu.VMEM((twos, 4, *group), BF16),
            pltpu.VMEM((comps, ghosts, nodes), BF16),
            pltpu.VMEM((2, levels, nodes), F32),
            pltpu.VMEM((levels, nodes), F32),
            pltpu.VMEM(group, BF16),
            pltpu.VMEM(group, BF16),
            pltpu.VMEM((ghosts, faces_n * ghosts), BF16),
            pltpu.VMEM((ghosts, nodes), F32),
            pltpu.VMEM((ghosts, wide), F32),
            pltpu.VMEM(group, F32),
            dma((10,)),
            dma((half, 4)),
            dma((half, 4)),
            dma((levels, 4)),
            dma((levels, 4)),
            dma((2, comps)),
            dma((2, 2, half)),
            dma((n_dev,)),
            dma((n_space,)),
            dma((2, 4)),
            dma((2, 4)),
            dma((2, half // 2, 4)),
            dma((twos, 16)),
            dma((twos, 16)),
            pltpu.SemaphoreType.REGULAR((max(1, len(rounds_of(n_space))), 2)),
            dma((2, 4)),
            dma(()),
        ],
        compiler_params=pltpu.CompilerParams(
            collective_id=0, has_side_effects=True, vmem_limit_bytes=60 * 1024 * 1024
        ),
        name="window",
    )(pitch, mixing, checkpoints, sources, metric, obj_weight, adjoint_end, lift, faces.T, send_idx)
    return pl.pallas_call(
        functools.partial(finish_kernel, comps),
        out_shape=(
            jax.ShapeDtypeStruct((1, *field), F32),
            jax.ShapeDtypeStruct((levels,), F32),
        ),
        in_specs=[anym] * 2,
        out_specs=(anym, anym),
        scratch_shapes=[pltpu.VMEM(field, F32), pltpu.VMEM((levels,), F32), dma((2, comps + 1))],
        compiler_params=pltpu.CompilerParams(vmem_limit_bytes=60 * 1024 * 1024),
        name="finish",
    )(bounds, grad)


def solution(mesh):
    placed = (
        P("tm", None, "space", None),
        P(None, None, "space", None),
        P(),
        P("space", None),
        P(None, "space", None),
        P(None, "space", None),
        P(),
        P(),
        P("space", None),
        P("space", None, None),
    )
    return jax.shard_map(
        shards,
        mesh=mesh,
        in_specs=placed,
        out_specs=(P("tm", None, "space", None), P()),
        check_vma=False,
    )
```
